32 devices in a mesh: beam: 8 (over y, x, core), hid: 4 (over z).
Axes of the slice: x: 2, y: 2, z: 4, core: 2. Of those that a mesh axis runs over, the one named last changes fastest.
Arguments:
- queries: bfloat16 [512, 256], P('beam'), may hold values from -6 to 6
- beam_ids: int32 [512, 256], P('beam'), may hold values from 0 to 131071, as said below
- child_table: bfloat16 [262144, 256], P('beam'), may hold values from -6 to 6
- w_query: bfloat16 [256, 1024], P(None, 'hid'), may hold values from -0.21875 to 0.21875
- w_child: bfloat16 [256, 1024], P(None, 'hid'), may hold values from -0.21875 to 0.21875
- w_cross: bfloat16 [256, 1024], P(None, 'hid'), may hold values from -0.21875 to 0.21875
- bias: float32 [1024], P('hid'), may hold values from -3 to 3
- w_out: float32 [1024], P('hid'), may hold values from -0.1875 to 0.1875
Outputs:
- scores: float32 [512, 512], P('beam', 'hid')
The draws below stay inside these ranges and needn't reach their ends.
Inputs may be any that keep to these rules, and one draw needn't show every extreme that they name: `beam_ids`: each id b names a node of the current level; its children are rows 2 b and 2 b + 1 of child_table. Among the ids of one index of beam's 64 queries, at most 3072 lie in the rows held by one index of beam (ids r * 16384 to (r + 1) * 16384 - 1 for index r), and in every draw one such index receives exactly 3072 from every index of beam.
All inputs are finite; a program needn't handle non-finite values.
Results may differ from the reference program's by a relative error of at most 0.0019.
Values may be sent and summed in bfloat16 or wider, within the bound.
No kernel may reach another device: no remote copies, remote signals or barrier semaphores. Data moves between devices by JAX's collectives and lax.ppermute only.
A program may use at most 128 MiB of HBM per device.

```python
import math
import jax
import jax.numpy as jnp
from jax import lax

E = 256
H = 1024
BEAM = 256
Q_DEV = 64
ROWS_DEV = 32768
QUERIES = 512
NODES = 262144
CAP = 3072
N_BEAM = 8


def draw_beam_ids(key, part):
    slots = Q_DEV * BEAM
    half = ROWS_DEV // 2
    hottest = jax.random.randint(jax.random.fold_in(key, 11), (), 0, N_BEAM)
    counter = jnp.arange(slots, dtype=jnp.int32)

    def one_block(block_key):
        others = hottest + 1 + (counter - CAP) % (N_BEAM - 1)
        owners = jnp.where(counter < CAP, hottest, others) % N_BEAM
        owners = jax.random.permutation(jax.random.fold_in(block_key, 2), owners)
        offsets = jax.random.randint(jax.random.fold_in(block_key, 3), (slots,), 0, half)
        return (owners * half + offsets).reshape(Q_DEV, BEAM)
    block_keys = jax.random.split(jax.random.fold_in(key, 4), N_BEAM)
    return jax.vmap(one_block)(block_keys).reshape(Q_DEV * N_BEAM, BEAM).astype(jnp.int32)


def block_levels(rng, extent, shards, low, high):
    gain = 1.0
    for position, parts in shards:
        steps = jax.random.uniform(jax.random.fold_in(jax.random.fold_in(rng, 6), position), (parts,), jnp.float32, low / len(shards), high / len(shards))
        gain = gain * jnp.repeat(jnp.exp(steps), extent[position] // parts).reshape((-1,) + (1,) * (len(extent) - 1 - position))
    return gain


def centred(key, extent, deviation, reach, pieces=(), held_as=jnp.bfloat16):
    values = jax.random.normal(key, extent, jnp.float32) * deviation
    if len(pieces) > 0:
        values = block_levels(key, extent, pieces, -0.22, 0.18) * values
    return jnp.clip(values, min=-reach, max=reach).astype(held_as)


def setup_inputs(seed: int = 0) -> dict:
    key_list = jax.random.split(jax.random.key(seed), 9)
    return {
        "queries": centred(key_list[0], (QUERIES, E), 1.0, 6.0, ((0, 8),)),
        "beam_ids": draw_beam_ids(jax.random.fold_in(key_list[8], 71), 0),
        "child_table": centred(key_list[2], (NODES, E), 1.0, 6.0, ((0, 8),)),
        "w_query": centred(key_list[3], (E, H), (3 * E) ** -0.5, 0.21875, ((1, 4),)),
        "w_child": centred(key_list[4], (E, H), (3 * E) ** -0.5, 0.21875, ((1, 4),)),
        "w_cross": centred(key_list[5], (E, H), (3 * E) ** -0.5, 0.21875, ((1, 4),)),
        "bias": centred(key_list[6], (H,), 0.5, 3.0, ((0, 4),), jnp.float32),
        "w_out": centred(key_list[7], (H,), H ** -0.5, 0.1875, ((0, 4),), jnp.float32),
    }


def reference(queries, beam_ids, child_table, w_query, w_child, w_cross, bias, w_out):
    pairs_table = child_table.reshape(NODES // 2, 2 * E)
    qproj = jnp.dot(queries, w_query, preferred_element_type=jnp.float32) + bias
    width = math.gcd(QUERIES, 16)
    count = QUERIES // width

    def score_block(packed):
        ids, qblock, pblock = packed
        rows = pairs_table[ids].reshape(width, 2 * BEAM, E)
        cross = (qblock[:, None, :].astype(jnp.float32) * rows.astype(jnp.float32)).astype(jnp.bfloat16)
        flat_rows = rows.reshape(width * 2 * BEAM, E)
        flat_cross = cross.reshape(width * 2 * BEAM, E)
        pre = jnp.dot(flat_rows, w_child, preferred_element_type=jnp.float32) + jnp.dot(flat_cross, w_cross, preferred_element_type=jnp.float32)
        pre = pre.reshape(width, 2 * BEAM, H) + pblock[:, None, :]
        return jnp.sum(jnp.maximum(pre, 0.0) * w_out, axis=-1)

    result = lax.map(score_block, (beam_ids.reshape(count, width, BEAM), queries.reshape(count, width, E), qproj.reshape(count, width, H)))
    return result.reshape(QUERIES, 2 * BEAM)
```

```python
import functools

import jax
import jax.numpy as jnp
from jax import lax
from jax.experimental import pallas as pl
from jax.experimental.pallas import tpu as pltpu
from jax.sharding import PartitionSpec as P

LANES = 128
TILES = 32
DIGITS = 3
ROWS = 128
OUT_SLOTS = 8
IN_SLOTS = 4
PIECE = 640


def iota(shape, dim):
    return lax.broadcasted_iota(jnp.int32, shape, dim)


def dot(a, b):
    return jnp.dot(a, b, preferred_element_type=jnp.float32)


def aligned(index, size):
    return pl.ds(pl.multiple_of(index, size), size)


def doubler():
    return (iota((2 * ROWS, ROWS), 0) >> 1 == iota((2 * ROWS, ROWS), 1)).astype(jnp.float32).astype(jnp.bfloat16)


def fetch_kernel(
    slots, embed, me_ref, x_ref, table_hbm,
    chunks_hbm, used_ref, name_ref, gidx,
    table, table_sem, eighths, insides, most_v, most_s, most_sem, rows_v, rows_sem, names_v, name_s, name_sem,
    q2f, work, work_sem, *rows_s,
):
    queries = x_ref.shape[0]
    blocks = queries // 8
    half = table_hbm.shape[0] * 4
    table_copy = pltpu.make_async_copy(table_hbm, table, table_sem)
    table_copy.start()

    lane = iota((ROWS, LANES), 1)
    lane8 = iota((8, LANES), 1)
    pick_row, pick_lane = iota((DIGITS * slots, LANES), 0), iota((DIGITS * slots, LANES), 1)
    spread = jnp.zeros((DIGITS * slots, LANES), jnp.float32)
    for digit in range(DIGITS):
        spread = jnp.where(pick_row == (pick_lane >> 1) + digit * slots, 256.0**digit, spread)
    spread = jnp.where(pick_lane < 2 * slots, spread, 0.0).astype(jnp.bfloat16)
    from_lane, to_lane = iota((LANES, LANES), 0), iota((LANES, LANES), 1)
    before = ((from_lane & 1) == 0) & ((from_lane >> 1) < (to_lane >> 1))
    before = before.astype(jnp.float32).astype(jnp.bfloat16)
    base = (me_ref[0] * half).astype(jnp.float32)
    twice = doubler()

    def compact(step, most):
        here = aligned(step * ROWS, ROWS)
        local = dot(x_ref[here, embed:], spread) - base
        owned = (local >= 0.0) & (local < float(half)) & (lane < 2 * slots)
        first = owned & ((lane & 1) == 0)
        mark = jnp.where(first, 1.0, 0.0)
        rank = dot(mark.astype(jnp.bfloat16), before).astype(jnp.int32)
        gidx[here, :] = jnp.where(owned, rank, -1)
        moved = jnp.where(first, ((lane - rank) << 16) + local.astype(jnp.int32), 0)
        for bit in range(7):
            other = pltpu.roll(moved, LANES - 2**bit, axis=1)
            flag = 65536 << bit
            moved = jnp.where((other & flag) != 0, other, jnp.where((moved & flag) != 0, 0, moved))
        total = jnp.broadcast_to(jnp.sum(mark, axis=1, keepdims=True), (ROWS, LANES)).astype(jnp.int32)
        eighth, inside = (moved & 65535) >> 2, (moved & 3) << 1
        for i in range(ROWS // 8):
            block = step * (ROWS // 8) + i
            to = aligned(block << 7, LANES)
            part = slice(i * 8, (i + 1) * 8)
            eighths[:, to] = eighth[part]
            insides[:, to] = inside[part] + (((block << 7) + lane8) << 3)
            most = jnp.where(lane8 == block, jnp.max(total[part], axis=0, keepdims=True), most)
        q2f[aligned(step * 2 * ROWS, 2 * ROWS), :] = dot(twice, x_ref[here, :embed])
        return most

    most_v[...] = lax.fori_loop(0, queries // ROWS, compact, jnp.zeros((8, LANES), jnp.int32))
    most_copy = pltpu.make_async_copy(most_v, most_s, most_sem)
    most_copy.start()
    most_copy.wait()

    zero = jnp.zeros((8, LANES), jnp.int32)

    def append(block, carry):
        used, held = carry
        more = most_s[0, block]
        turn, low = used & (LANES - 1), used >> 7
        crossed = turn + more >= LANES
        kept = []
        for source, target, last in zip((eighths, insides), (rows_v, names_v), held):
            rolled = pltpu.roll(source[:, aligned(block << 7, LANES)], turn, axis=1)
            merged = jnp.where(lane8 >= turn, rolled, last)
            target[:, aligned(low << 7, LANES)] = merged
            kept.append(jnp.where(crossed, rolled, merged))
        return used + more, tuple(kept)

    used, held = lax.fori_loop(0, blocks, append, (0, (zero, zero)), unroll=8)
    for target, last in zip((rows_v, names_v), held):
        target[:, aligned((used >> 7) << 7, LANES)] = last
    chunks = (used + TILES - 1) >> (TILES.bit_length() - 1)
    used_ref[0] = chunks
    name_ref[...] = names_v[0:1, :]

    def scalar_copies(act):
        for start in range(0, names_v.shape[1], PIECE):
            here = pl.ds(start, min(PIECE, names_v.shape[1] - start))

            @pl.when(start < chunks * TILES)
            def _():
                for s in range(8):
                    act(pltpu.make_async_copy(rows_v.at[pl.ds(s, 1), here], rows_s[s].at[:, here], rows_sem.at[s]))
                act(pltpu.make_async_copy(names_v.at[pl.ds(0, 1), here], name_s.at[:, here], name_sem))

    scalar_copies(lambda copy: copy.start())
    scalar_copies(lambda copy: copy.wait())
    table_copy.wait()

    pair = iota((8, LANES), 0) >> 1
    child = iota((8, LANES), 0) & 1

    def out_copy(number):
        slot = number & (OUT_SLOTS - 1)
        return pltpu.make_async_copy(work.at[slot], chunks_hbm.at[number], work_sem.at[slot])

    def chunk(number, carry):
        slot = number & (OUT_SLOTS - 1)

        @pl.when(number >= OUT_SLOTS)
        def _():
            out_copy(number - OUT_SLOTS).wait()

        def tile(t, carry):
            at = number * TILES + t
            block = name_s[0, at] >> 10
            names = names_v[:, aligned((at >> 7) << 7, LANES)]
            starts = jnp.take_along_axis(names, jnp.broadcast_to(at & (LANES - 1), (8, LANES)), axis=1) & 7
            halves = []
            for part in range(2):
                place = jnp.take_along_axis(starts, pair + 4 * part, axis=0) + child
                got = [None] * (embed // LANES)
                for s in range(4):
                    eight = table[rows_s[part * 4 + s][0, at]].astype(jnp.float32)
                    for j in range(embed // LANES):
                        piece = jnp.take_along_axis(eight[:, j * LANES : (j + 1) * LANES], place, axis=0)
                        got[j] = piece if s == 0 else jnp.where(pair == s, piece, got[j])
                halves.append(jnp.concatenate(got, axis=1))
            rows = jnp.concatenate(halves, axis=0)
            here = aligned(t << 4, 16)
            work[slot, here, :embed] = rows.astype(jnp.bfloat16)
            work[slot, here, embed:] = (rows * q2f[aligned(block << 4, 16), :]).astype(jnp.bfloat16)
            return carry

        lax.fori_loop(0, TILES, tile, 0, unroll=TILES)
        out_copy(number).start()
        return carry

    lax.fori_loop(0, chunks, chunk, 0)

    def drain(number, carry):
        out_copy(number).wait()
        return carry

    lax.fori_loop(jnp.maximum(chunks - OUT_SLOTS, 0), chunks, drain, 0)


def fetch(me, x, table, slots, embed):
    queries = x.shape[0]
    blocks = queries // 8
    tiles = -(-(blocks * slots + 2 * LANES) // LANES) * LANES
    vmem = pl.BlockSpec(memory_space=pltpu.VMEM)
    smem = pl.BlockSpec(memory_space=pltpu.SMEM)
    anywhere = pl.BlockSpec(memory_space=pl.ANY)
    i32 = jnp.int32
    return pl.pallas_call(
        functools.partial(fetch_kernel, slots, embed),
        out_shape=(
            jax.ShapeDtypeStruct((blocks * slots // TILES, TILES * 16, 2 * embed), jnp.bfloat16),
            jax.ShapeDtypeStruct((1,), i32),
            jax.ShapeDtypeStruct((1, tiles), i32),
            jax.ShapeDtypeStruct((queries, LANES), i32),
        ),
        in_specs=[smem, vmem, anywhere],
        out_specs=(anywhere, smem, vmem, vmem),
        scratch_shapes=[
            pltpu.VMEM(table.shape, table.dtype),
            pltpu.SemaphoreType.DMA(()),
            pltpu.VMEM((8, blocks * LANES), i32),
            pltpu.VMEM((8, blocks * LANES), i32),
            pltpu.VMEM((8, LANES), i32),
            pltpu.SMEM((8, LANES), i32),
            pltpu.SemaphoreType.DMA(()),
            pltpu.VMEM((8, tiles), i32),
            pltpu.SemaphoreType.DMA((8,)),
            pltpu.VMEM((8, tiles), i32),
            pltpu.SMEM((1, tiles), i32),
            pltpu.SemaphoreType.DMA(()),
            pltpu.VMEM((2 * queries, embed), jnp.float32),
            pltpu.VMEM((OUT_SLOTS, TILES * 16, 2 * embed), jnp.bfloat16),
            pltpu.SemaphoreType.DMA((OUT_SLOTS,)),
        ]
        + [pltpu.SMEM((1, tiles), i32)] * 8,
        cost_estimate=pl.CostEstimate(flops=2 * 10**10, bytes_accessed=4 * 10**7, transcendentals=0),
        name="fetch",
    )(me, x, table)


def score_kernel(embed, used_ref, names_s, x_ref, gidx, chunks_hbm, *rest):
    count = len(rest) - 7
    weights = rest[:count]
    out_ref, held, held_sem, qp2, work, work_sem, scores = rest[count:]
    queries = x_ref.shape[0]
    hidden = weights[0].shape[1]
    copies = [pltpu.make_async_copy(weights[k], held.at[k], held_sem.at[k]) for k in range(count)]
    for copy in copies:
        copy.start()
    chunks = used_ref[0]

    def in_copy(number):
        slot = number & (IN_SLOTS - 1)
        return pltpu.make_async_copy(chunks_hbm.at[number], work.at[slot], work_sem.at[slot])

    for number in range(IN_SLOTS - 1):

        @pl.when(number < chunks)
        def _():
            in_copy(number).start()

    for copy in copies:
        copy.wait()

    twice = doubler()

    def project(step, carry):
        here = aligned(step * 2 * ROWS, 2 * ROWS)
        doubled = dot(twice, x_ref[aligned(step * ROWS, ROWS), :embed]).astype(jnp.bfloat16)
        for k in range(count):
            last = held[k, 3 * embed :, :].astype(jnp.float32)
            bias = last[0:1] + last[1:2] + last[2:3]
            qp2[here, k * hidden : (k + 1) * hidden] = dot(doubled, held[k, 2 * embed : 3 * embed, :]) + bias
        return carry

    lax.fori_loop(0, queries // ROWS, project, 0)

    lane16 = iota((16, LANES), 1)

    def score_chunk(number, carry):
        ahead = number + IN_SLOTS - 1

        @pl.when(ahead < chunks)
        def _():
            in_copy(ahead).start()

        in_copy(number).wait()
        rows = work.at[number & (IN_SLOTS - 1)]
        sums = [None] * TILES
        for k in range(count):
            last = held[k, 3 * embed :, :].astype(jnp.float32)
            scale = last[3:4] + last[4:5] + last[5:6]
            pre = dot(rows[...], held[k, : 2 * embed, :])
            for t in range(TILES):
                block = names_s[0, number * TILES + t] >> 10
                own = qp2[aligned(block << 4, 16), k * hidden : (k + 1) * hidden]
                act = jnp.maximum(pre[t * 16 : (t + 1) * 16] + own, 0.0) * scale
                for j in range(0, hidden, LANES):
                    part = act[:, j : j + LANES]
                    sums[t] = part if sums[t] is None else sums[t] + part
        for t in range(TILES):
            name = names_s[0, number * TILES + t]
            here = aligned((name >> 10) << 4, 16)
            rank = (name >> 3) & (LANES - 1)
            total = jnp.sum(sums[t], axis=1, keepdims=True)
            scores[here, :] = jnp.where(lane16 == rank, total, scores[here, :])
        return carry

    lax.fori_loop(0, chunks, score_chunk, 0)

    lane8 = iota((8, LANES), 1)

    def place(block, carry):
        here = aligned(block << 3, 8)
        index = gidx[here, :]
        safe = jnp.maximum(index, 0)
        left = jnp.take_along_axis(scores[pl.ds(block * 16, 8, stride=2), :], safe, axis=1)
        right = jnp.take_along_axis(scores[pl.ds(block * 16 + 1, 8, stride=2), :], safe, axis=1)
        out_ref[here, :] = jnp.where(index < 0, 0.0, jnp.where((lane8 & 1) == 0, left, right))
        return carry

    lax.fori_loop(0, queries // 8, place, 0, unroll=8)


def score(used, names, x, gidx, chunks, weights, embed):
    queries = x.shape[0]
    depth, hidden = weights[0].shape
    vmem = pl.BlockSpec(memory_space=pltpu.VMEM)
    smem = pl.BlockSpec(memory_space=pltpu.SMEM)
    anywhere = pl.BlockSpec(memory_space=pl.ANY)
    return pl.pallas_call(
        functools.partial(score_kernel, embed),
        out_shape=jax.ShapeDtypeStruct((queries, LANES), jnp.float32),
        in_specs=[smem, smem, vmem, vmem, anywhere] + [anywhere] * len(weights),
        out_specs=vmem,
        scratch_shapes=[
            pltpu.VMEM((len(weights), depth, hidden), jnp.bfloat16),
            pltpu.SemaphoreType.DMA((len(weights),)),
            pltpu.VMEM((2 * queries, len(weights) * hidden), jnp.float32),
            pltpu.VMEM((IN_SLOTS, TILES * 16, 2 * embed), jnp.bfloat16),
            pltpu.SemaphoreType.DMA((IN_SLOTS,)),
            pltpu.VMEM((2 * queries, LANES), jnp.float32),
        ],
        name="score",
    )(used, names, x, gidx, chunks, *weights)


def thirds(x):
    high = lax.reduce_precision(x, 8, 7)
    middle = lax.reduce_precision(x - high, 8, 7)
    low = lax.reduce_precision(x - high - middle, 8, 7)
    return [high, middle, low]


def shards(queries, beam_ids, child_table, w_query, w_child, w_cross, bias, w_out):
    nbeam, nhid = lax.axis_size("beam"), lax.axis_size("hid")
    qcount, width = beam_ids.shape
    embed = queries.shape[1]
    slots = width // nhid
    half = child_table.shape[0] // 2
    assert 2 * slots <= LANES and half <= 65536 and half * nbeam <= 256**DIGITS and qcount * nbeam <= 8 * LANES

    tail = jnp.stack(thirds(bias) + thirds(w_out) + [jnp.zeros_like(bias)] * 10).astype(jnp.bfloat16)
    own = jnp.concatenate([w_child, w_cross, w_query, tail], axis=0)
    weights = [own]
    for shift in range(1, nhid):
        weights.append(lax.ppermute(own, "hid", [(i, (i + shift) % nhid) for i in range(nhid)]))

    mine = lax.dynamic_slice_in_dim(beam_ids, lax.axis_index("hid") * slots, slots, 1)
    digits = [(mine >> (8 * digit)) & 255 for digit in range(DIGITS)]
    x = jnp.concatenate([queries] + [d.astype(jnp.bfloat16) for d in digits], axis=1)
    x = lax.all_gather(x, "beam", axis=0, tiled=True)

    me = lax.axis_index("beam").astype(jnp.int32).reshape(1)
    chunks, used, names, gidx = fetch(me, x, child_table.reshape(-1, 8, embed), slots, embed)
    found = score(used, names, x, gidx, chunks, weights, embed)[:, : 2 * slots]
    parts = lax.all_to_all(found.reshape(nbeam, qcount, 2 * slots), "beam", split_axis=0, concat_axis=0, tiled=True)
    return jnp.sum(parts, axis=0)


def solution(mesh):
    return jax.shard_map(
        shards,
        mesh=mesh,
        in_specs=(
            P("beam", None),
            P("beam", None),
            P("beam", None),
            P(None, "hid"),
            P(None, "hid"),
            P(None, "hid"),
            P("hid"),
            P("hid"),
        ),
        out_specs=P("beam", "hid"),
        check_vma=False,
    )
```

```python
import functools

import jax
import jax.numpy as jnp
from jax import lax
from jax.experimental import pallas as pl
from jax.experimental.pallas import tpu as pltpu
from jax.sharding import PartitionSpec as P

LANES = 128
TILES = 32
DIGITS = 2
BASE = 512
ROWS = 128
OUT_SLOTS = 8
IN_SLOTS = 4
PIECE = 640


def iota(shape, dim):
    return lax.broadcasted_iota(jnp.int32, shape, dim)


def dot(a, b):
    return jnp.dot(a, b, preferred_element_type=jnp.float32)


def aligned(index, size):
    return pl.ds(pl.multiple_of(index, size), size)


def doubler():
    return (iota((2 * ROWS, ROWS), 0) >> 1 == iota((2 * ROWS, ROWS), 1)).astype(jnp.float32).astype(jnp.bfloat16)


def fetch_kernel(
    slots, embed, me_ref, x_ref, table_hbm,
    chunks_hbm, used_ref, name_ref, gidx,
    table, table_sem, eighths, insides, most_v, most_s, most_sem, rows_v, rows_sem, names_v, name_s, name_sem,
    q2f, work, work_sem, *rows_s,
):
    queries = x_ref.shape[0]
    blocks = queries // 8
    half = table_hbm.shape[0] * 4
    table_copy = pltpu.make_async_copy(table_hbm, table, table_sem)
    table_copy.start()

    lane = iota((ROWS, LANES), 1)
    lane8 = iota((8, LANES), 1)
    pick_row, pick_lane = iota((DIGITS * slots, LANES), 0), iota((DIGITS * slots, LANES), 1)
    spread = jnp.zeros((DIGITS * slots, LANES), jnp.float32)
    for digit in range(DIGITS):
        spread = jnp.where(pick_row == (pick_lane >> 1) + digit * slots, float(BASE) ** digit, spread)
    spread = jnp.where(pick_lane < 2 * slots, spread, 0.0).astype(jnp.bfloat16)
    from_lane, to_lane = iota((LANES, LANES), 0), iota((LANES, LANES), 1)
    before = ((from_lane & 1) == 0) & ((from_lane >> 1) < (to_lane >> 1))
    before = before.astype(jnp.float32).astype(jnp.bfloat16)
    base = (me_ref[0] * half).astype(jnp.float32) - sum(BASE // 2 * BASE**digit for digit in range(DIGITS))
    twice = doubler()

    def compact(step, most):
        here = aligned(step * ROWS, ROWS)
        local = dot(x_ref[here, embed:], spread) - base
        owned = (local >= 0.0) & (local < float(half)) & (lane < 2 * slots)
        first = owned & ((lane & 1) == 0)
        mark = jnp.where(first, 1.0, 0.0)
        rank = dot(mark.astype(jnp.bfloat16), before).astype(jnp.int32)
        gidx[here, :] = jnp.where(owned, rank, -1)
        moved = jnp.where(first, ((lane - rank) << 16) + local.astype(jnp.int32), 0)
        for bit in range(7):
            other = pltpu.roll(moved, LANES - 2**bit, axis=1)
            flag = 65536 << bit
            moved = jnp.where((other & flag) != 0, other, jnp.where((moved & flag) != 0, 0, moved))
        total = jnp.broadcast_to(jnp.sum(mark, axis=1, keepdims=True), (ROWS, LANES)).astype(jnp.int32)
        eighth, inside = (moved & 65535) >> 2, (moved & 3) << 1
        for i in range(ROWS // 8):
            block = step * (ROWS // 8) + i
            to = aligned(block << 7, LANES)
            part = slice(i * 8, (i + 1) * 8)
            eighths[:, to] = eighth[part]
            insides[:, to] = inside[part] + (((block << 7) + lane8) << 3)
            most = jnp.where(lane8 == block, jnp.max(total[part], axis=0, keepdims=True), most)
        q2f[aligned(step * 2 * ROWS, 2 * ROWS), :] = dot(twice, x_ref[here, :embed])
        return most

    most_v[...] = lax.fori_loop(0, queries // ROWS, compact, jnp.zeros((8, LANES), jnp.int32))
    most_copy = pltpu.make_async_copy(most_v, most_s, most_sem)
    most_copy.start()
    most_copy.wait()

    zero = jnp.zeros((8, LANES), jnp.int32)

    def append(block, carry):
        used, held = carry
        more = most_s[0, block]
        turn, low = used & (LANES - 1), used >> 7
        crossed = turn + more >= LANES
        kept = []
        for source, target, last in zip((eighths, insides), (rows_v, names_v), held):
            rolled = pltpu.roll(source[:, aligned(block << 7, LANES)], turn, axis=1)
            merged = jnp.where(lane8 >= turn, rolled, last)
            target[:, aligned(low << 7, LANES)] = merged
            kept.append(jnp.where(crossed, rolled, merged))
        return used + more, tuple(kept)

    used, held = lax.fori_loop(0, blocks, append, (0, (zero, zero)), unroll=8)
    for target, last in zip((rows_v, names_v), held):
        target[:, aligned((used >> 7) << 7, LANES)] = last
    chunks = (used + TILES - 1) >> (TILES.bit_length() - 1)
    used_ref[0] = chunks
    name_ref[...] = names_v[0:1, :]

    def scalar_copies(act):
        for start in range(0, names_v.shape[1], PIECE):
            here = pl.ds(start, min(PIECE, names_v.shape[1] - start))

            @pl.when(start < chunks * TILES)
            def _():
                for s in range(8):
                    act(pltpu.make_async_copy(rows_v.at[pl.ds(s, 1), here], rows_s[s].at[:, here], rows_sem.at[s]))
                act(pltpu.make_async_copy(names_v.at[pl.ds(0, 1), here], name_s.at[:, here], name_sem))

    scalar_copies(lambda copy: copy.start())
    scalar_copies(lambda copy: copy.wait())
    table_copy.wait()

    pair = iota((8, LANES), 0) >> 1
    child = iota((8, LANES), 0) & 1

    def out_copy(number):
        slot = number & (OUT_SLOTS - 1)
        return pltpu.make_async_copy(work.at[slot], chunks_hbm.at[number], work_sem.at[slot])

    def chunk(number, carry):
        slot = number & (OUT_SLOTS - 1)

        @pl.when(number >= OUT_SLOTS)
        def _():
            out_copy(number - OUT_SLOTS).wait()

        def tile(t, carry):
            at = number * TILES + t
            block = name_s[0, at] >> 10
            names = names_v[:, aligned((at >> 7) << 7, LANES)]
            starts = jnp.take_along_axis(names, jnp.broadcast_to(at & (LANES - 1), (8, LANES)), axis=1) & 7
            halves = []
            for part in range(2):
                place = jnp.take_along_axis(starts, pair + 4 * part, axis=0) + child
                got = [None] * (embed // LANES)
                for s in range(4):
                    eight = table[rows_s[part * 4 + s][0, at]].astype(jnp.float32)
                    for j in range(embed // LANES):
                        piece = jnp.take_along_axis(eight[:, j * LANES : (j + 1) * LANES], place, axis=0)
                        got[j] = piece if s == 0 else jnp.where(pair == s, piece, got[j])
                halves.append(jnp.concatenate(got, axis=1))
            rows = jnp.concatenate(halves, axis=0)
            here = aligned(t << 4, 16)
            work[slot, here, :embed] = rows.astype(jnp.bfloat16)
            work[slot, here, embed:] = (rows * q2f[aligned(block << 4, 16), :]).astype(jnp.bfloat16)
            return carry

        lax.fori_loop(0, TILES, tile, 0, unroll=TILES)
        out_copy(number).start()
        return carry

    lax.fori_loop(0, chunks, chunk, 0)

    def drain(number, carry):
        out_copy(number).wait()
        return carry

    lax.fori_loop(jnp.maximum(chunks - OUT_SLOTS, 0), chunks, drain, 0)


def fetch(me, x, table, slots, embed):
    queries = x.shape[0]
    blocks = queries // 8
    tiles = -(-(blocks * slots + 2 * LANES) // LANES) * LANES
    vmem = pl.BlockSpec(memory_space=pltpu.VMEM)
    smem = pl.BlockSpec(memory_space=pltpu.SMEM)
    anywhere = pl.BlockSpec(memory_space=pl.ANY)
    i32 = jnp.int32
    return pl.pallas_call(
        functools.partial(fetch_kernel, slots, embed),
        out_shape=(
            jax.ShapeDtypeStruct((blocks * slots // TILES, TILES * 16, 2 * embed), jnp.bfloat16),
            jax.ShapeDtypeStruct((1,), i32),
            jax.ShapeDtypeStruct((1, tiles), i32),
            jax.ShapeDtypeStruct((queries, LANES), i32),
        ),
        in_specs=[smem, vmem, anywhere],
        out_specs=(anywhere, smem, vmem, vmem),
        scratch_shapes=[
            pltpu.VMEM(table.shape, table.dtype),
            pltpu.SemaphoreType.DMA(()),
            pltpu.VMEM((8, blocks * LANES), i32),
            pltpu.VMEM((8, blocks * LANES), i32),
            pltpu.VMEM((8, LANES), i32),
            pltpu.SMEM((8, LANES), i32),
            pltpu.SemaphoreType.DMA(()),
            pltpu.VMEM((8, tiles), i32),
            pltpu.SemaphoreType.DMA((8,)),
            pltpu.VMEM((8, tiles), i32),
            pltpu.SMEM((1, tiles), i32),
            pltpu.SemaphoreType.DMA(()),
            pltpu.VMEM((2 * queries, embed), jnp.float32),
            pltpu.VMEM((OUT_SLOTS, TILES * 16, 2 * embed), jnp.bfloat16),
            pltpu.SemaphoreType.DMA((OUT_SLOTS,)),
        ]
        + [pltpu.SMEM((1, tiles), i32)] * 8,
        cost_estimate=pl.CostEstimate(flops=2 * 10**10, bytes_accessed=4 * 10**7, transcendentals=0),
        name="fetch",
    )(me, x, table)


def score_kernel(embed, used_ref, name_s, x_ref, gidx, chunks_hbm, *rest):
    count = len(rest) - 9
    weights = rest[:count]
    out_ref, held, held_sem, qp2, work, work_sem, scores, pending, sums = rest[count:]
    queries = x_ref.shape[0]
    hidden = weights[0].shape[1]
    copies = [pltpu.make_async_copy(weights[k], held.at[k], held_sem.at[k]) for k in range(count)]
    for copy in copies:
        copy.start()
    chunks = used_ref[0]

    def in_copy(number):
        slot = number & (IN_SLOTS - 1)
        return pltpu.make_async_copy(chunks_hbm.at[number], work.at[slot], work_sem.at[slot])

    for number in range(IN_SLOTS - 1):

        @pl.when(number < chunks)
        def _():
            in_copy(number).start()

    for copy in copies:
        copy.wait()

    twice = doubler()

    def project(step, carry):
        here = aligned(step * 2 * ROWS, 2 * ROWS)
        doubled = dot(twice, x_ref[aligned(step * ROWS, ROWS), :embed]).astype(jnp.bfloat16)
        for k in range(count):
            last = held[k, 3 * embed :, :].astype(jnp.float32)
            bias = last[0:1] + last[1:2] + last[2:3]
            qp2[here, k * hidden : (k + 1) * hidden] = dot(doubled, held[k, 2 * embed : 3 * embed, :]) + bias
        return carry

    lax.fori_loop(0, queries // ROWS, project, 0, unroll=4)

    lane16 = iota((16, LANES), 1)

    def scale_of(k):
        last = held[k, 3 * embed :, :].astype(jnp.float32)
        return last[3:4] + last[4:5] + last[5:6]

    def activate(pre, name, k):
        own = qp2[aligned((name >> 10) << 4, 16), k * hidden : (k + 1) * hidden]
        act = jnp.maximum(pre + own, 0.0) * scales[k]
        total = act[:, :LANES]
        for j in range(LANES, hidden, LANES):
            total = total + act[:, j : j + LANES]
        return total

    def finish(number):
        for t in range(TILES):
            name = name_s[0, number * TILES + t]
            part = slice(t * 16, (t + 1) * 16)
            total = activate(pending[part, :], name, count - 1)
            if count > 1:
                total = total + sums[part, :]
            here = aligned((name >> 10) << 4, 16)
            rank = (name >> 3) & (LANES - 1)
            scores[here, :] = jnp.where(lane16 == rank, jnp.sum(total, axis=1, keepdims=True), scores[here, :])

    scales = [scale_of(k) for k in range(count)]

    def score_chunk(number, carry):
        ahead = number + IN_SLOTS - 1

        @pl.when(ahead < chunks)
        def _():
            in_copy(ahead).start()

        in_copy(number).wait()
        rows = work.at[number & (IN_SLOTS - 1)]
        totals = [None] * TILES
        for k in range(count - 1):
            pre = dot(rows[...], held[k, : 2 * embed, :])
            if k == 0:
                finish(jnp.maximum(number - 1, 0))
            for t in range(TILES):
                own = activate(pre[t * 16 : (t + 1) * 16], name_s[0, number * TILES + t], k)
                totals[t] = own if k == 0 else totals[t] + own
        if count > 1:
            for t in range(TILES):
                sums[t * 16 : (t + 1) * 16, :] = totals[t]
        pending[...] = dot(rows[...], held[count - 1, : 2 * embed, :])
        return carry

    lax.fori_loop(0, chunks, score_chunk, 0)
    finish(jnp.maximum(chunks - 1, 0))

    lane8 = iota((8, LANES), 1)

    def place(block):
        index = gidx[aligned(block << 3, 8), :]
        safe = jnp.maximum(index, 0)
        left = jnp.take_along_axis(scores[pl.ds(block * 16, 8, stride=2), :], safe, axis=1)
        right = jnp.take_along_axis(scores[pl.ds(block * 16 + 1, 8, stride=2), :], safe, axis=1)
        return jnp.where(index < 0, 0.0, jnp.where((lane8 & 1) == 0, left, right))

    def place_two(two, carry):
        both = jnp.concatenate([place(2 * two), place(2 * two + 1)], axis=0)
        out_ref[aligned(two << 4, 16), :] = both.astype(out_ref.dtype)
        return carry

    lax.fori_loop(0, queries // 16, place_two, 0, unroll=4)


def score(used, names, x, gidx, chunks, weights, embed):
    queries = x.shape[0]
    depth, hidden = weights[0].shape
    vmem = pl.BlockSpec(memory_space=pltpu.VMEM)
    smem = pl.BlockSpec(memory_space=pltpu.SMEM)
    anywhere = pl.BlockSpec(memory_space=pl.ANY)
    return pl.pallas_call(
        functools.partial(score_kernel, embed),
        out_shape=jax.ShapeDtypeStruct((queries, LANES), jnp.float32),
        in_specs=[smem, smem, vmem, vmem, anywhere] + [anywhere] * len(weights),
        out_specs=vmem,
        scratch_shapes=[
            pltpu.VMEM((len(weights), depth, hidden), jnp.bfloat16),
            pltpu.SemaphoreType.DMA((len(weights),)),
            pltpu.VMEM((2 * queries, len(weights) * hidden), jnp.float32),
            pltpu.VMEM((IN_SLOTS, TILES * 16, 2 * embed), jnp.bfloat16),
            pltpu.SemaphoreType.DMA((IN_SLOTS,)),
            pltpu.VMEM((2 * queries, LANES), jnp.float32),
            pltpu.VMEM((TILES * 16, hidden), jnp.float32),
            pltpu.VMEM((TILES * 16, LANES), jnp.float32),
        ],
        name="score",
    )(used, names, x, gidx, chunks, *weights)


def prepare_kernel(slots, place_ref, queries, ids, child, cross, query, bias, scale, own, x):
    embed = queries.shape[1]
    for k, w in enumerate((child, cross, query)):
        own[k * embed : (k + 1) * embed, :] = w[...]
    row = iota((16, own.shape[1]), 0)
    tail = jnp.zeros((16, own.shape[1]), jnp.float32)
    for k, value in enumerate((bias, scale)):
        left = value[...]
        for part in range(3):
            taken = left.astype(jnp.bfloat16).astype(jnp.float32)
            tail = jnp.where(row == 3 * k + part, taken, tail)
            left = left - taken
    own[3 * embed :, :] = tail.astype(jnp.bfloat16)
    shape = (ids.shape[1], DIGITS * slots)
    digits = None
    for digit in range(DIGITS):
        value = ((ids[...] >> (digit * (BASE.bit_length() - 1))) & (BASE - 1)) - BASE // 2
        pick = iota(shape, 0) - place_ref[0] * slots == iota(shape, 1) - digit * slots
        pick = pick & (iota(shape, 1) >= digit * slots) & (iota(shape, 1) < (digit + 1) * slots)
        part = dot(value.astype(jnp.float32).astype(jnp.bfloat16), pick.astype(jnp.float32).astype(jnp.bfloat16))
        digits = part if digits is None else digits + part
    x[:, :embed] = queries[...]
    x[:, embed:] = digits.astype(jnp.bfloat16)


def prepare(queries, ids, child, cross, query, bias, scale, slots):
    embed, hidden = child.shape
    vmem = pl.BlockSpec(memory_space=pltpu.VMEM)
    place = lax.axis_index("hid").astype(jnp.int32).reshape(1)
    return pl.pallas_call(
        functools.partial(prepare_kernel, slots),
        out_shape=(
            jax.ShapeDtypeStruct((3 * embed + 16, hidden), jnp.bfloat16),
            jax.ShapeDtypeStruct((queries.shape[0], embed + DIGITS * slots), jnp.bfloat16),
        ),
        in_specs=[pl.BlockSpec(memory_space=pltpu.SMEM)] + [vmem] * 7,
        out_specs=(vmem, vmem),
        name="prepare",
    )(place, queries, ids, child, cross, query, bias.reshape(1, -1), scale.reshape(1, -1))


def shards(queries, beam_ids, child_table, w_query, w_child, w_cross, bias, w_out):
    nbeam, nhid = lax.axis_size("beam"), lax.axis_size("hid")
    qcount, width = beam_ids.shape
    embed = queries.shape[1]
    slots = width // nhid
    half = child_table.shape[0] // 2
    assert 2 * slots <= LANES and half <= 65536 and half * nbeam <= BASE**DIGITS and qcount * nbeam <= 8 * LANES

    own, x = prepare(queries, beam_ids, w_child, w_cross, w_query, bias, w_out, slots)
    weights = [own]
    for shift in range(1, nhid):
        weights.append(lax.ppermute(own, "hid", [(i, (i + shift) % nhid) for i in range(nhid)]))
    x = lax.all_gather(x, "beam", axis=0, tiled=True)

    me = lax.axis_index("beam").astype(jnp.int32).reshape(1)
    chunks, used, names, gidx = fetch(me, x, child_table.reshape(-1, 8, embed), slots, embed)
    found = score(used, names, x, gidx, chunks, weights, embed)[:, : 2 * slots]
    parts = lax.all_to_all(found.reshape(nbeam, qcount, 2 * slots), "beam", split_axis=0, concat_axis=0, tiled=True)
    return jnp.sum(parts, axis=0)


def solution(mesh):
    return jax.shard_map(
        shards,
        mesh=mesh,
        in_specs=(
            P("beam", None),
            P("beam", None),
            P("beam", None),
            P(None, "hid"),
            P(None, "hid"),
            P(None, "hid"),
            P("hid"),
            P("hid"),
        ),
        out_specs=P("beam", "hid"),
        check_vma=False,
    )
```

```python
import functools

import jax
import jax.numpy as jnp
from jax import lax
from jax.experimental import pallas as pl
from jax.experimental.pallas import tpu as pltpu
from jax.sharding import PartitionSpec as P

LANES = 128
TILES = 32
DIGITS = 2
BASE = 512
ROWS = 128
OUT_SLOTS = 8
IN_SLOTS = 4
PIECE = 640


def iota(shape, dim):
    return lax.broadcasted_iota(jnp.int32, shape, dim)


def dot(a, b):
    return jnp.dot(a, b, preferred_element_type=jnp.float32)


def aligned(index, size):
    return pl.ds(pl.multiple_of(index, size), size)


def doubler():
    return (iota((2 * ROWS, ROWS), 0) >> 1 == iota((2 * ROWS, ROWS), 1)).astype(jnp.float32).astype(jnp.bfloat16)


def fetch_kernel(
    slots, embed, me_ref, x_ref, table_hbm,
    chunks_hbm, used_ref, name_ref, gidx, order_ref, sorted_ref,
    table, table_sem, eighths, insides, most_v, most_s, most_sem, rows_v, rows_sem, names_v, name_s, name_sem,
    q2f, work, work_sem, *rows_s,
):
    queries = x_ref.shape[0]
    blocks = queries // 8
    half = table_hbm.shape[0] * 4
    table_copy = pltpu.make_async_copy(table_hbm, table, table_sem)
    table_copy.start()

    lane = iota((ROWS, LANES), 1)
    lane8 = iota((8, LANES), 1)
    pick_row, pick_lane = iota((DIGITS * slots, LANES), 0), iota((DIGITS * slots, LANES), 1)
    spread = jnp.zeros((DIGITS * slots, LANES), jnp.float32)
    for digit in range(DIGITS):
        spread = jnp.where(pick_row == (pick_lane >> 1) + digit * slots, float(BASE) ** digit, spread)
    spread = jnp.where(pick_lane < 2 * slots, spread, 0.0).astype(jnp.bfloat16)
    from_lane, to_lane = iota((LANES, LANES), 0), iota((LANES, LANES), 1)
    before = ((from_lane & 1) == 0) & ((from_lane >> 1) < (to_lane >> 1))
    before = before.astype(jnp.float32).astype(jnp.bfloat16)
    base = (me_ref[0] * half).astype(jnp.float32) - sum(BASE // 2 * BASE**digit for digit in range(DIGITS))
    twice = doubler()

    def owned_of(digits):
        local = dot(digits, spread) - base
        mine = (local >= 0.0) & (local < float(half)) & (iota(local.shape, 1) < 2 * slots)
        return local, mine

    mark = jnp.where(owned_of(x_ref[:, embed:])[1] & ((iota((queries, LANES), 1) & 1) == 0), 1.0, 0.0)
    number = jnp.sum(mark, axis=1, keepdims=True)
    across = lax.dot_general(
        jnp.ones((8, LANES), jnp.bfloat16), mark.astype(jnp.bfloat16), (((1,), (1,)), ((), ())),
        preferred_element_type=jnp.float32,
    )[0:1]
    earlier = iota((queries, queries), 1) < iota((queries, queries), 0)
    ahead = (across > number) | ((across == number) & earlier)
    order = jnp.sum(ahead.astype(jnp.float32), axis=1, keepdims=True).astype(jnp.int32)
    order_ref[...] = jnp.broadcast_to(order, (queries, LANES))
    later = iota((queries, queries), 0) < iota((queries, queries), 1)
    behind = (number > across) | ((number == across) & later)
    place = jnp.sum(behind.astype(jnp.float32), axis=0, keepdims=True).astype(jnp.int32)
    move = (iota((queries, queries), 0) == place).astype(jnp.float32).astype(jnp.bfloat16)
    sorted_ref[...] = dot(move, x_ref[...]).astype(jnp.bfloat16)

    def compact(step, most):
        here = aligned(step * ROWS, ROWS)
        local, owned = owned_of(sorted_ref[here, embed:])
        first = owned & ((lane & 1) == 0)
        mark = jnp.where(first, 1.0, 0.0)
        rank = dot(mark.astype(jnp.bfloat16), before).astype(jnp.int32)
        gidx[here, :] = jnp.where(owned, rank, -1)
        moved = jnp.where(first, ((lane - rank) << 16) + local.astype(jnp.int32), 0)
        for bit in range(7):
            other = pltpu.roll(moved, LANES - 2**bit, axis=1)
            flag = 65536 << bit
            moved = jnp.where((other & flag) != 0, other, jnp.where((moved & flag) != 0, 0, moved))
        total = jnp.broadcast_to(jnp.sum(mark, axis=1, keepdims=True), (ROWS, LANES)).astype(jnp.int32)
        eighth, inside = (moved & 65535) >> 2, (moved & 3) << 1
        for i in range(ROWS // 8):
            block = step * (ROWS // 8) + i
            to = aligned(block << 7, LANES)
            part = slice(i * 8, (i + 1) * 8)
            eighths[:, to] = eighth[part]
            insides[:, to] = inside[part] + (((block << 7) + lane8) << 3)
            most = jnp.where(lane8 == block, jnp.max(total[part], axis=0, keepdims=True), most)
        q2f[aligned(step * 2 * ROWS, 2 * ROWS), :] = dot(twice, sorted_ref[here, :embed])
        return most

    most_v[...] = lax.fori_loop(0, queries // ROWS, compact, jnp.zeros((8, LANES), jnp.int32))
    most_copy = pltpu.make_async_copy(most_v, most_s, most_sem)
    most_copy.start()
    most_copy.wait()

    zero = jnp.zeros((8, LANES), jnp.int32)

    def append(block, carry):
        used, held = carry
        more = most_s[0, block]
        turn, low = used & (LANES - 1), used >> 7
        crossed = turn + more >= LANES
        kept = []
        for source, target, last in zip((eighths, insides), (rows_v, names_v), held):
            rolled = pltpu.roll(source[:, aligned(block << 7, LANES)], turn, axis=1)
            merged = jnp.where(lane8 >= turn, rolled, last)
            target[:, aligned(low << 7, LANES)] = merged
            kept.append(jnp.where(crossed, rolled, merged))
        return used + more, tuple(kept)

    used, held = lax.fori_loop(0, blocks, append, (0, (zero, zero)), unroll=8)
    for target, last in zip((rows_v, names_v), held):
        target[:, aligned((used >> 7) << 7, LANES)] = last
    chunks = (used + TILES - 1) >> (TILES.bit_length() - 1)
    used_ref[0] = chunks
    name_ref[...] = names_v[0:1, :]

    def scalar_copies(act):
        for start in range(0, names_v.shape[1], PIECE):
            here = pl.ds(start, min(PIECE, names_v.shape[1] - start))

            @pl.when(start < chunks * TILES)
            def _():
                for s in range(8):
                    act(pltpu.make_async_copy(rows_v.at[pl.ds(s, 1), here], rows_s[s].at[:, here], rows_sem.at[s]))
                act(pltpu.make_async_copy(names_v.at[pl.ds(0, 1), here], name_s.at[:, here], name_sem))

    scalar_copies(lambda copy: copy.start())
    scalar_copies(lambda copy: copy.wait())
    table_copy.wait()

    pair = iota((8, LANES), 0) >> 1
    child = iota((8, LANES), 0) & 1

    def out_copy(number):
        slot = number & (OUT_SLOTS - 1)
        return pltpu.make_async_copy(work.at[slot], chunks_hbm.at[number], work_sem.at[slot])

    def chunk(number, carry):
        slot = number & (OUT_SLOTS - 1)

        @pl.when(number >= OUT_SLOTS)
        def _():
            out_copy(number - OUT_SLOTS).wait()

        def tile(t, carry):
            at = number * TILES + t
            block = name_s[0, at] >> 10
            names = names_v[:, aligned((at >> 7) << 7, LANES)]
            starts = jnp.take_along_axis(names, jnp.broadcast_to(at & (LANES - 1), (8, LANES)), axis=1) & 7
            halves = []
            for part in range(2):
                place = jnp.take_along_axis(starts, pair + 4 * part, axis=0) + child
                got = [None] * (embed // LANES)
                for s in range(4):
                    eight = table[rows_s[part * 4 + s][0, at]].astype(jnp.float32)
                    for j in range(embed // LANES):
                        piece = jnp.take_along_axis(eight[:, j * LANES : (j + 1) * LANES], place, axis=0)
                        got[j] = piece if s == 0 else jnp.where(pair == s, piece, got[j])
                halves.append(jnp.concatenate(got, axis=1))
            rows = jnp.concatenate(halves, axis=0)
            here = aligned(t << 4, 16)
            work[slot, here, :embed] = rows.astype(jnp.bfloat16)
            work[slot, here, embed:] = (rows * q2f[aligned(block << 4, 16), :]).astype(jnp.bfloat16)
            return carry

        lax.fori_loop(0, TILES, tile, 0, unroll=TILES)
        out_copy(number).start()
        return carry

    lax.fori_loop(0, chunks, chunk, 0)

    def drain(number, carry):
        out_copy(number).wait()
        return carry

    lax.fori_loop(jnp.maximum(chunks - OUT_SLOTS, 0), chunks, drain, 0)


def fetch(me, x, table, slots, embed):
    queries = x.shape[0]
    blocks = queries // 8
    tiles = -(-(blocks * slots + 2 * LANES) // LANES) * LANES
    vmem = pl.BlockSpec(memory_space=pltpu.VMEM)
    smem = pl.BlockSpec(memory_space=pltpu.SMEM)
    anywhere = pl.BlockSpec(memory_space=pl.ANY)
    i32 = jnp.int32
    return pl.pallas_call(
        functools.partial(fetch_kernel, slots, embed),
        out_shape=(
            jax.ShapeDtypeStruct((blocks * slots // TILES, TILES * 16, 2 * embed), jnp.bfloat16),
            jax.ShapeDtypeStruct((1,), i32),
            jax.ShapeDtypeStruct((1, tiles), i32),
            jax.ShapeDtypeStruct((queries, LANES), i32),
            jax.ShapeDtypeStruct((queries, LANES), i32),
            jax.ShapeDtypeStruct(x.shape, x.dtype),
        ),
        in_specs=[smem, vmem, anywhere],
        out_specs=(anywhere, smem, vmem, vmem, vmem, vmem),
        scratch_shapes=[
            pltpu.VMEM(table.shape, table.dtype),
            pltpu.SemaphoreType.DMA(()),
            pltpu.VMEM((8, blocks * LANES), i32),
            pltpu.VMEM((8, blocks * LANES), i32),
            pltpu.VMEM((8, LANES), i32),
            pltpu.SMEM((8, LANES), i32),
            pltpu.SemaphoreType.DMA(()),
            pltpu.VMEM((8, tiles), i32),
            pltpu.SemaphoreType.DMA((8,)),
            pltpu.VMEM((8, tiles), i32),
            pltpu.SMEM((1, tiles), i32),
            pltpu.SemaphoreType.DMA(()),
            pltpu.VMEM((2 * queries, embed), jnp.float32),
            pltpu.VMEM((OUT_SLOTS, TILES * 16, 2 * embed), jnp.bfloat16),
            pltpu.SemaphoreType.DMA((OUT_SLOTS,)),
        ]
        + [pltpu.SMEM((1, tiles), i32)] * 8,
        cost_estimate=pl.CostEstimate(flops=2 * 10**10, bytes_accessed=4 * 10**7, transcendentals=0),
        name="fetch",
    )(me, x, table)


def score_kernel(embed, used_ref, name_s, x_ref, gidx, order_ref, chunks_hbm, *rest):
    count = len(rest) - 10
    weights = rest[:count]
    out_ref, held, held_sem, qp2, work, work_sem, scores, pending, sums, placed = rest[count:]
    queries = x_ref.shape[0]
    hidden = weights[0].shape[1]
    copies = [pltpu.make_async_copy(weights[k], held.at[k], held_sem.at[k]) for k in range(count)]
    for copy in copies:
        copy.start()
    chunks = used_ref[0]

    def in_copy(number):
        slot = number & (IN_SLOTS - 1)
        return pltpu.make_async_copy(chunks_hbm.at[number], work.at[slot], work_sem.at[slot])

    for number in range(IN_SLOTS - 1):

        @pl.when(number < chunks)
        def _():
            in_copy(number).start()

    for copy in copies:
        copy.wait()

    twice = doubler()

    def project(step, carry):
        here = aligned(step * 2 * ROWS, 2 * ROWS)
        doubled = dot(twice, x_ref[aligned(step * ROWS, ROWS), :embed]).astype(jnp.bfloat16)
        for k in range(count):
            last = held[k, 3 * embed :, :].astype(jnp.float32)
            bias = last[0:1] + last[1:2] + last[2:3]
            qp2[here, k * hidden : (k + 1) * hidden] = dot(doubled, held[k, 2 * embed : 3 * embed, :]) + bias
        return carry

    lax.fori_loop(0, queries // ROWS, project, 0, unroll=4)

    lane16 = iota((16, LANES), 1)

    def scale_of(k):
        last = held[k, 3 * embed :, :].astype(jnp.float32)
        return last[3:4] + last[4:5] + last[5:6]

    def activate(pre, name, k):
        own = qp2[aligned((name >> 10) << 4, 16), k * hidden : (k + 1) * hidden]
        act = jnp.maximum(pre + own, 0.0) * scales[k]
        total = act[:, :LANES]
        for j in range(LANES, hidden, LANES):
            total = total + act[:, j : j + LANES]
        return total

    def finish(number):
        for t in range(TILES):
            name = name_s[0, number * TILES + t]
            part = slice(t * 16, (t + 1) * 16)
            total = activate(pending[part, :], name, count - 1)
            if count > 1:
                total = total + sums[part, :]
            here = aligned((name >> 10) << 4, 16)
            rank = (name >> 3) & (LANES - 1)
            scores[here, :] = jnp.where(lane16 == rank, jnp.sum(total, axis=1, keepdims=True), scores[here, :])

    scales = [scale_of(k) for k in range(count)]

    def score_chunk(number, carry):
        ahead = number + IN_SLOTS - 1

        @pl.when(ahead < chunks)
        def _():
            in_copy(ahead).start()

        in_copy(number).wait()
        rows = work.at[number & (IN_SLOTS - 1)]
        totals = [None] * TILES
        for k in range(count - 1):
            pre = dot(rows[...], held[k, : 2 * embed, :])
            if k == 0:
                finish(jnp.maximum(number - 1, 0))
            for t in range(TILES):
                own = activate(pre[t * 16 : (t + 1) * 16], name_s[0, number * TILES + t], k)
                totals[t] = own if k == 0 else totals[t] + own
        if count > 1:
            for t in range(TILES):
                sums[t * 16 : (t + 1) * 16, :] = totals[t]
        pending[...] = dot(rows[...], held[count - 1, : 2 * embed, :])
        return carry

    lax.fori_loop(0, chunks, score_chunk, 0)
    finish(jnp.maximum(chunks - 1, 0))

    lane8 = iota((8, LANES), 1)

    def place(block):
        index = gidx[aligned(block << 3, 8), :]
        safe = jnp.maximum(index, 0)
        left = jnp.take_along_axis(scores[pl.ds(block * 16, 8, stride=2), :], safe, axis=1)
        right = jnp.take_along_axis(scores[pl.ds(block * 16 + 1, 8, stride=2), :], safe, axis=1)
        return jnp.where(index < 0, 0.0, jnp.where((lane8 & 1) == 0, left, right))

    def place_block(block, carry):
        placed[aligned(block << 3, 8), :] = place(block)
        return carry

    lax.fori_loop(0, queries // 8, place_block, 0, unroll=8)

    move = (order_ref[:, 0:1] == iota((queries, queries), 1)).astype(jnp.float32).astype(jnp.bfloat16)
    left = placed[...]
    moved = None
    for _ in range(3):
        taken = left.astype(jnp.bfloat16)
        left = left - taken.astype(jnp.float32)
        part = dot(move, taken)
        moved = part if moved is None else moved + part
    out_ref[...] = moved


def score(used, names, x, gidx, order, chunks, weights, embed):
    queries = x.shape[0]
    depth, hidden = weights[0].shape
    vmem = pl.BlockSpec(memory_space=pltpu.VMEM)
    smem = pl.BlockSpec(memory_space=pltpu.SMEM)
    anywhere = pl.BlockSpec(memory_space=pl.ANY)
    return pl.pallas_call(
        functools.partial(score_kernel, embed),
        out_shape=jax.ShapeDtypeStruct((queries, LANES), jnp.float32),
        in_specs=[smem, smem, vmem, vmem, vmem, anywhere] + [anywhere] * len(weights),
        out_specs=vmem,
        scratch_shapes=[
            pltpu.VMEM((len(weights), depth, hidden), jnp.bfloat16),
            pltpu.SemaphoreType.DMA((len(weights),)),
            pltpu.VMEM((2 * queries, len(weights) * hidden), jnp.float32),
            pltpu.VMEM((IN_SLOTS, TILES * 16, 2 * embed), jnp.bfloat16),
            pltpu.SemaphoreType.DMA((IN_SLOTS,)),
            pltpu.VMEM((2 * queries, LANES), jnp.float32),
            pltpu.VMEM((TILES * 16, hidden), jnp.float32),
            pltpu.VMEM((TILES * 16, LANES), jnp.float32),
            pltpu.VMEM((queries, LANES), jnp.float32),
        ],
        name="score",
    )(used, names, x, gidx, order, chunks, *weights)


def prepare_kernel(slots, place_ref, queries, ids, child, cross, query, bias, scale, own, x):
    embed = queries.shape[1]
    for k, w in enumerate((child, cross, query)):
        own[k * embed : (k + 1) * embed, :] = w[...]
    row = iota((16, own.shape[1]), 0)
    tail = jnp.zeros((16, own.shape[1]), jnp.float32)
    for k, value in enumerate((bias, scale)):
        left = value[...]
        for part in range(3):
            taken = left.astype(jnp.bfloat16).astype(jnp.float32)
            tail = jnp.where(row == 3 * k + part, taken, tail)
            left = left - taken
    own[3 * embed :, :] = tail.astype(jnp.bfloat16)
    shape = (ids.shape[1], DIGITS * slots)
    digits = None
    for digit in range(DIGITS):
        value = ((ids[...] >> (digit * (BASE.bit_length() - 1))) & (BASE - 1)) - BASE // 2
        pick = iota(shape, 0) - place_ref[0] * slots == iota(shape, 1) - digit * slots
        pick = pick & (iota(shape, 1) >= digit * slots) & (iota(shape, 1) < (digit + 1) * slots)
        part = dot(value.astype(jnp.float32).astype(jnp.bfloat16), pick.astype(jnp.float32).astype(jnp.bfloat16))
        digits = part if digits is None else digits + part
    x[:, :embed] = queries[...]
    x[:, embed:] = digits.astype(jnp.bfloat16)


def prepare(queries, ids, child, cross, query, bias, scale, slots):
    embed, hidden = child.shape
    vmem = pl.BlockSpec(memory_space=pltpu.VMEM)
    place = lax.axis_index("hid").astype(jnp.int32).reshape(1)
    return pl.pallas_call(
        functools.partial(prepare_kernel, slots),
        out_shape=(
            jax.ShapeDtypeStruct((3 * embed + 16, hidden), jnp.bfloat16),
            jax.ShapeDtypeStruct((queries.shape[0], embed + DIGITS * slots), jnp.bfloat16),
        ),
        in_specs=[pl.BlockSpec(memory_space=pltpu.SMEM)] + [vmem] * 7,
        out_specs=(vmem, vmem),
        name="prepare",
    )(place, queries, ids, child, cross, query, bias.reshape(1, -1), scale.reshape(1, -1))


def shards(queries, beam_ids, child_table, w_query, w_child, w_cross, bias, w_out):
    nbeam, nhid = lax.axis_size("beam"), lax.axis_size("hid")
    qcount, width = beam_ids.shape
    embed = queries.shape[1]
    slots = width // nhid
    half = child_table.shape[0] // 2
    assert 2 * slots <= LANES and half <= 65536 and half * nbeam <= BASE**DIGITS and qcount * nbeam <= 8 * LANES

    own, x = prepare(queries, beam_ids, w_child, w_cross, w_query, bias, w_out, slots)
    weights = [own]
    for shift in range(1, nhid):
        weights.append(lax.ppermute(own, "hid", [(i, (i + shift) % nhid) for i in range(nhid)]))
    x = lax.all_gather(x, "beam", axis=0, tiled=True)

    me = lax.axis_index("beam").astype(jnp.int32).reshape(1)
    chunks, used, names, gidx, order, x = fetch(me, x, child_table.reshape(-1, 8, embed), slots, embed)
    found = score(used, names, x, gidx, order, chunks, weights, embed)[:, : 2 * slots]
    parts = lax.all_to_all(found.reshape(nbeam, qcount, 2 * slots), "beam", split_axis=0, concat_axis=0, tiled=True)
    return jnp.sum(parts, axis=0)


def solution(mesh):
    return jax.shard_map(
        shards,
        mesh=mesh,
        in_specs=(
            P("beam", None),
            P("beam", None),
            P("beam", None),
            P(None, "hid"),
            P(None, "hid"),
            P(None, "hid"),
            P("hid"),
            P("hid"),
        ),
        out_specs=P("beam", "hid"),
        check_vma=False,
    )
```

```python
import functools

import jax
import jax.numpy as jnp
from jax import lax
from jax.experimental import pallas as pl
from jax.experimental.pallas import tpu as pltpu
from jax.sharding import PartitionSpec as P

LANES = 128
TILES = 32
DIGITS = 2
BASE = 512
ROWS = 256
OUT_SLOTS = 8
IN_SLOTS = 4
GROUP = 2 * TILES
PIECE = 896


def iota(shape, dim):
    return lax.broadcasted_iota(jnp.int32, shape, dim)


def dot(a, b):
    return jnp.dot(a, b, preferred_element_type=jnp.float32)


def aligned(index, size):
    return pl.ds(pl.multiple_of(index, size), size)


def doubler():
    return (iota((2 * ROWS, ROWS), 0) >> 1 == iota((2 * ROWS, ROWS), 1)).astype(jnp.float32).astype(jnp.bfloat16)


def fetch_kernel(
    slots, embed, me_ref, x_ref, table_hbm,
    chunks_hbm, used_ref, name_hbm, gidx_hbm, order_hbm, sorted_hbm,
    name_ref, gidx, order_ref, sorted_ref, side_sem, table, table_sem, eighths, insides, most_v, most_s, most_sem, rows_v, rows_sem, names_v, name_s, name_sem,
    q2f, work, work_sem, *rows_s,
):
    queries = x_ref.shape[0]
    blocks = queries // 8
    half = table_hbm.shape[0] * 4
    table_copy = pltpu.make_async_copy(table_hbm, table, table_sem)
    table_copy.start()

    lane = iota((ROWS, LANES), 1)
    lane8 = iota((8, LANES), 1)
    pick_row, pick_lane = iota((DIGITS * slots, LANES), 0), iota((DIGITS * slots, LANES), 1)
    spread = jnp.zeros((DIGITS * slots, LANES), jnp.float32)
    for digit in range(DIGITS):
        spread = jnp.where(pick_row == (pick_lane >> 1) + digit * slots, float(BASE) ** digit, spread)
    spread = jnp.where(pick_lane < 2 * slots, spread, 0.0).astype(jnp.bfloat16)
    from_lane, to_lane = iota((LANES, LANES), 0), iota((LANES, LANES), 1)
    before = ((from_lane & 1) == 0) & ((from_lane >> 1) < (to_lane >> 1))
    before = before.astype(jnp.float32).astype(jnp.bfloat16)
    base = (me_ref[0] * half).astype(jnp.float32) - sum(BASE // 2 * BASE**digit for digit in range(DIGITS))
    twice = doubler()

    def owned_of(digits):
        local = dot(digits, spread) - base
        mine = (local >= 0.0) & (local < float(half)) & (iota(local.shape, 1) < 2 * slots)
        return local, mine

    mark = jnp.where(owned_of(x_ref[:, embed:])[1] & ((iota((queries, LANES), 1) & 1) == 0), 1.0, 0.0)
    number = jnp.sum(mark, axis=1, keepdims=True)
    across = lax.dot_general(
        jnp.ones((8, LANES), jnp.bfloat16), mark.astype(jnp.bfloat16), (((1,), (1,)), ((), ())),
        preferred_element_type=jnp.float32,
    )[0:1]
    earlier = iota((queries, queries), 1) < iota((queries, queries), 0)
    ahead = (across > number) | ((across == number) & earlier)
    order = jnp.sum(ahead.astype(jnp.float32), axis=1, keepdims=True).astype(jnp.int32)
    order_ref[...] = jnp.broadcast_to(order, (queries, LANES))
    later = iota((queries, queries), 0) < iota((queries, queries), 1)
    behind = (number > across) | ((number == across) & later)
    place = jnp.sum(behind.astype(jnp.float32), axis=0, keepdims=True).astype(jnp.int32)
    move = (iota((queries, queries), 0) == place).astype(jnp.float32).astype(jnp.bfloat16)
    sorted_ref[...] = dot(move, x_ref[...]).astype(jnp.bfloat16)
    sides = [
        pltpu.make_async_copy(value, target, side_sem.at[i])
        for i, (value, target) in enumerate(
            ((order_ref, order_hbm), (sorted_ref, sorted_hbm), (gidx, gidx_hbm), (name_ref, name_hbm))
        )
    ]
    sides[0].start()
    sides[1].start()

    def compact(step, most):
        here = aligned(step * ROWS, ROWS)
        local, owned = owned_of(sorted_ref[here, embed:])
        first = owned & ((lane & 1) == 0)
        mark = jnp.where(first, 1.0, 0.0)
        rank = dot(mark.astype(jnp.bfloat16), before).astype(jnp.int32)
        gidx[here, :] = jnp.where(owned, rank, -1)
        moved = jnp.where(first, ((lane - rank) << 16) + local.astype(jnp.int32), 0)
        for bit in range(7):
            other = pltpu.roll(moved, LANES - 2**bit, axis=1)
            flag = 65536 << bit
            moved = jnp.where((other & flag) != 0, other, jnp.where((moved & flag) != 0, 0, moved))
        total = jnp.broadcast_to(jnp.sum(mark, axis=1, keepdims=True), (ROWS, LANES)).astype(jnp.int32)
        eighth, inside = (moved & 65535) >> 2, (moved & 3) << 1
        for i in range(ROWS // 8):
            block = step * (ROWS // 8) + i
            to = aligned(block << 7, LANES)
            part = slice(i * 8, (i + 1) * 8)
            eighths[:, to] = eighth[part]
            insides[:, to] = inside[part] + (((block << 7) + lane8) << 3)
            most = jnp.where(lane8 == block, jnp.max(total[part], axis=0, keepdims=True), most)
        q2f[aligned(step * 2 * ROWS, 2 * ROWS), :] = dot(twice, sorted_ref[here, :embed])
        return most

    most_v[...] = lax.fori_loop(0, queries // ROWS, compact, jnp.zeros((8, LANES), jnp.int32))
    most_copy = pltpu.make_async_copy(most_v, most_s, most_sem)
    most_copy.start()
    sides[2].start()
    most_copy.wait()

    zero = jnp.zeros((8, LANES), jnp.int32)

    def append(block, carry):
        used, held = carry
        more = most_s[0, block]
        turn, low = used & (LANES - 1), used >> 7
        crossed = turn + more >= LANES
        kept = []
        for source, target, last in zip((eighths, insides), (rows_v, names_v), held):
            rolled = pltpu.roll(source[:, aligned(block << 7, LANES)], turn, axis=1)
            merged = jnp.where(lane8 >= turn, rolled, last)
            target[:, aligned(low << 7, LANES)] = merged
            kept.append(jnp.where(crossed, rolled, merged))
        return used + more, tuple(kept)

    used, held = lax.fori_loop(0, blocks, append, (0, (zero, zero)), unroll=8)
    for target, last in zip((rows_v, names_v), held):
        target[:, aligned((used >> 7) << 7, LANES)] = last
    chunks = (used + TILES - 1) >> (TILES.bit_length() - 1)
    used_ref[0] = chunks
    name_ref[...] = names_v[0:1, :]
    sides[3].start()

    def scalar_copies(act):
        for start in range(0, names_v.shape[1], PIECE):
            here = pl.ds(start, min(PIECE, names_v.shape[1] - start))

            @pl.when(start < chunks * TILES)
            def _():
                for s in range(8):
                    act(pltpu.make_async_copy(rows_v.at[pl.ds(s, 1), here], rows_s[s].at[:, here], rows_sem.at[s]))
                act(pltpu.make_async_copy(names_v.at[pl.ds(0, 1), here], name_s.at[:, here], name_sem))

    scalar_copies(lambda copy: copy.start())
    scalar_copies(lambda copy: copy.wait())
    table_copy.wait()

    pair = iota((8, LANES), 0) >> 1
    child = iota((8, LANES), 0) & 1

    def out_copy(number):
        slot = number & (OUT_SLOTS - 1)
        return pltpu.make_async_copy(work.at[slot], chunks_hbm.at[number], work_sem.at[slot])

    def chunk(number, carry):
        slot = number & (OUT_SLOTS - 1)

        @pl.when(number >= OUT_SLOTS)
        def _():
            out_copy(number - OUT_SLOTS).wait()

        def tile(t, carry):
            at = number * TILES + t
            block = name_s[0, at] >> 10
            names = names_v[:, aligned((at >> 7) << 7, LANES)]
            starts = jnp.take_along_axis(names, jnp.broadcast_to(at & (LANES - 1), (8, LANES)), axis=1) & 7
            halves = []
            for part in range(2):
                place = jnp.take_along_axis(starts, pair + 4 * part, axis=0) + child
                got = [None] * (embed // LANES)
                for s in range(4):
                    eight = table[rows_s[part * 4 + s][0, at]].astype(jnp.float32)
                    for j in range(embed // LANES):
                        piece = jnp.take_along_axis(eight[:, j * LANES : (j + 1) * LANES], place, axis=0)
                        got[j] = piece if s == 0 else jnp.where(pair == s, piece, got[j])
                halves.append(jnp.concatenate(got, axis=1))
            rows = jnp.concatenate(halves, axis=0)
            here = aligned(t << 4, 16)
            work[slot, here, :embed] = rows.astype(jnp.bfloat16)
            work[slot, here, embed:] = (rows * q2f[aligned(block << 4, 16), :]).astype(jnp.bfloat16)
            return carry

        lax.fori_loop(0, TILES, tile, 0, unroll=TILES)
        out_copy(number).start()
        return carry

    lax.fori_loop(0, chunks, chunk, 0)

    def drain(number, carry):
        out_copy(number).wait()
        return carry

    lax.fori_loop(jnp.maximum(chunks - OUT_SLOTS, 0), chunks, drain, 0)
    for side in sides:
        side.wait()


def fetch(me, x, table, slots, embed):
    queries = x.shape[0]
    blocks = queries // 8
    tiles = -(-(blocks * slots + 2 * LANES) // LANES) * LANES
    vmem = pl.BlockSpec(memory_space=pltpu.VMEM)
    smem = pl.BlockSpec(memory_space=pltpu.SMEM)
    anywhere = pl.BlockSpec(memory_space=pl.ANY)
    i32 = jnp.int32
    return pl.pallas_call(
        functools.partial(fetch_kernel, slots, embed),
        out_shape=(
            jax.ShapeDtypeStruct((blocks * slots // TILES, TILES * 16, 2 * embed), jnp.bfloat16),
            jax.ShapeDtypeStruct((1,), i32),
            jax.ShapeDtypeStruct((1, tiles), i32),
            jax.ShapeDtypeStruct((queries, LANES), i32),
            jax.ShapeDtypeStruct((queries, LANES), i32),
            jax.ShapeDtypeStruct(x.shape, x.dtype),
        ),
        in_specs=[smem, vmem, anywhere],
        out_specs=(anywhere, smem, anywhere, anywhere, anywhere, anywhere),
        scratch_shapes=[
            pltpu.VMEM((1, tiles), i32),
            pltpu.VMEM((queries, LANES), i32),
            pltpu.VMEM((queries, LANES), i32),
            pltpu.VMEM(x.shape, x.dtype),
            pltpu.SemaphoreType.DMA((4,)),
            pltpu.VMEM(table.shape, table.dtype),
            pltpu.SemaphoreType.DMA(()),
            pltpu.VMEM((8, blocks * LANES), i32),
            pltpu.VMEM((8, blocks * LANES), i32),
            pltpu.VMEM((8, LANES), i32),
            pltpu.SMEM((8, LANES), i32),
            pltpu.SemaphoreType.DMA(()),
            pltpu.VMEM((8, tiles), i32),
            pltpu.SemaphoreType.DMA((8,)),
            pltpu.VMEM((8, tiles), i32),
            pltpu.SMEM((1, tiles), i32),
            pltpu.SemaphoreType.DMA(()),
            pltpu.VMEM((2 * queries, embed), jnp.float32),
            pltpu.VMEM((OUT_SLOTS, TILES * 16, 2 * embed), jnp.bfloat16),
            pltpu.SemaphoreType.DMA((OUT_SLOTS,)),
        ]
        + [pltpu.SMEM((1, tiles), i32)] * 8,
        cost_estimate=pl.CostEstimate(flops=2 * 10**10, bytes_accessed=4 * 10**7, transcendentals=0),
        name="fetch",
    )(me, x, table)


def score_kernel(embed, used_ref, name_s, x_hbm, gidx_hbm, order_hbm, chunks_hbm, *rest):
    count = len(rest) - 14
    weights = rest[:count]
    out_ref, x_ref, gidx, order_ref, side_sem, held, held_sem, qp2, work, work_sem, scores, pending, sums, placed = rest[count:]
    queries = x_hbm.shape[0]
    hidden = weights[0].shape[1]
    sides = [
        pltpu.make_async_copy(source, value, side_sem.at[i])
        for i, (source, value) in enumerate(((x_hbm, x_ref), (gidx_hbm, gidx), (order_hbm, order_ref)))
    ]
    sides[0].start()
    copies = [pltpu.make_async_copy(weights[k], held.at[k], held_sem.at[k]) for k in range(count)]
    for copy in copies:
        copy.start()
    chunks = (used_ref[0] * TILES + GROUP - 1) // GROUP

    def in_copy(number):
        slot = number & (IN_SLOTS - 1)
        return pltpu.make_async_copy(chunks_hbm.at[number], work.at[slot], work_sem.at[slot])

    for number in range(IN_SLOTS - 1):

        @pl.when(number < chunks)
        def _():
            in_copy(number).start()

    for copy in copies:
        copy.wait()

    for side in sides[1:]:
        side.start()
    sides[0].wait()

    twice = doubler()

    def project(step, carry):
        here = aligned(step * 2 * ROWS, 2 * ROWS)
        doubled = dot(twice, x_ref[aligned(step * ROWS, ROWS), :embed]).astype(jnp.bfloat16)
        for k in range(count):
            last = held[k, 3 * embed :, :].astype(jnp.float32)
            bias = last[0:1] + last[1:2] + last[2:3]
            qp2[here, k * hidden : (k + 1) * hidden] = dot(doubled, held[k, 2 * embed : 3 * embed, :]) + bias
        return carry

    lax.fori_loop(0, queries // ROWS, project, 0, unroll=2)

    lane16 = iota((16, LANES), 1)

    def scale_of(k):
        last = held[k, 3 * embed :, :].astype(jnp.float32)
        return last[3:4] + last[4:5] + last[5:6]

    def activate(pre, name, k):
        own = qp2[aligned((name >> 10) << 4, 16), k * hidden : (k + 1) * hidden]
        act = jnp.maximum(pre + own, 0.0) * scales[k]
        total = act[:, :LANES]
        for j in range(LANES, hidden, LANES):
            total = total + act[:, j : j + LANES]
        return total

    def finish(number):
        for t in range(GROUP):
            name = name_s[0, number * GROUP + t]
            part = slice(t * 16, (t + 1) * 16)
            total = activate(pending[part, :], name, count - 1)
            if count > 1:
                total = total + sums[part, :]
            here = aligned((name >> 10) << 4, 16)
            rank = (name >> 3) & (LANES - 1)
            scores[here, :] = jnp.where(lane16 == rank, jnp.sum(total, axis=1, keepdims=True), scores[here, :])

    scales = [scale_of(k) for k in range(count)]

    def score_chunk(number, carry):
        ahead = number + IN_SLOTS - 1

        @pl.when(ahead < chunks)
        def _():
            in_copy(ahead).start()

        in_copy(number).wait()
        rows = work.at[number & (IN_SLOTS - 1)]
        totals = [None] * GROUP
        for k in range(count - 1):
            pre = dot(rows[...], held[k, : 2 * embed, :])
            if k == 0:
                finish(jnp.maximum(number - 1, 0))
            for t in range(GROUP):
                own = activate(pre[t * 16 : (t + 1) * 16], name_s[0, number * GROUP + t], k)
                totals[t] = own if k == 0 else totals[t] + own
        if count > 1:
            for t in range(GROUP):
                sums[t * 16 : (t + 1) * 16, :] = totals[t]
        pending[...] = dot(rows[...], held[count - 1, : 2 * embed, :])
        return carry

    lax.fori_loop(0, chunks, score_chunk, 0)
    finish(jnp.maximum(chunks - 1, 0))

    for side in sides[1:]:
        side.wait()
    lane8 = iota((8, LANES), 1)

    def place(block):
        index = gidx[aligned(block << 3, 8), :]
        safe = jnp.maximum(index, 0)
        left = jnp.take_along_axis(scores[pl.ds(block * 16, 8, stride=2), :], safe, axis=1)
        right = jnp.take_along_axis(scores[pl.ds(block * 16 + 1, 8, stride=2), :], safe, axis=1)
        return jnp.where(index < 0, 0.0, jnp.where((lane8 & 1) == 0, left, right))

    def place_block(block, carry):
        placed[aligned(block << 3, 8), :] = place(block)
        return carry

    lax.fori_loop(0, queries // 8, place_block, 0, unroll=8)

    move = (order_ref[:, 0:1] == iota((queries, queries), 1)).astype(jnp.float32).astype(jnp.bfloat16)
    left = placed[...]
    moved = None
    for _ in range(3):
        taken = left.astype(jnp.bfloat16)
        left = left - taken.astype(jnp.float32)
        part = dot(move, taken)
        moved = part if moved is None else moved + part
    out_ref[...] = moved


def score(used, names, x, gidx, order, chunks, weights, embed):
    queries = x.shape[0]
    depth, hidden = weights[0].shape
    vmem = pl.BlockSpec(memory_space=pltpu.VMEM)
    smem = pl.BlockSpec(memory_space=pltpu.SMEM)
    anywhere = pl.BlockSpec(memory_space=pl.ANY)
    return pl.pallas_call(
        functools.partial(score_kernel, embed),
        out_shape=jax.ShapeDtypeStruct((queries, LANES), jnp.float32),
        in_specs=[smem, smem, anywhere, anywhere, anywhere, anywhere] + [anywhere] * len(weights),
        out_specs=vmem,
        scratch_shapes=[
            pltpu.VMEM(x.shape, x.dtype),
            pltpu.VMEM((queries, LANES), jnp.int32),
            pltpu.VMEM((queries, LANES), jnp.int32),
            pltpu.SemaphoreType.DMA((3,)),
            pltpu.VMEM((len(weights), depth, hidden), jnp.bfloat16),
            pltpu.SemaphoreType.DMA((len(weights),)),
            pltpu.VMEM((2 * queries, len(weights) * hidden), jnp.float32),
            pltpu.VMEM((IN_SLOTS, GROUP * 16, 2 * embed), jnp.bfloat16),
            pltpu.SemaphoreType.DMA((IN_SLOTS,)),
            pltpu.VMEM((2 * queries, LANES), jnp.float32),
            pltpu.VMEM((GROUP * 16, hidden), jnp.float32),
            pltpu.VMEM((GROUP * 16, LANES), jnp.float32),
            pltpu.VMEM((queries, LANES), jnp.float32),
        ],
        name="score",
    )(used, names, x, gidx, order, chunks.reshape(-1, GROUP * 16, 2 * embed), *weights)


def prepare_kernel(slots, place_ref, queries, ids, child, cross, query, bias, scale, own, x):
    embed = queries.shape[1]
    for k, w in enumerate((child, cross, query)):
        own[k * embed : (k + 1) * embed, :] = w[...]
    row = iota((16, own.shape[1]), 0)
    tail = jnp.zeros((16, own.shape[1]), jnp.float32)
    for k, value in enumerate((bias, scale)):
        left = value[...]
        for part in range(3):
            taken = left.astype(jnp.bfloat16).astype(jnp.float32)
            tail = jnp.where(row == 3 * k + part, taken, tail)
            left = left - taken
    own[3 * embed :, :] = tail.astype(jnp.bfloat16)
    shape = (ids.shape[1], DIGITS * slots)
    digits = None
    for digit in range(DIGITS):
        value = ((ids[...] >> (digit * (BASE.bit_length() - 1))) & (BASE - 1)) - BASE // 2
        pick = iota(shape, 0) - place_ref[0] * slots == iota(shape, 1) - digit * slots
        pick = pick & (iota(shape, 1) >= digit * slots) & (iota(shape, 1) < (digit + 1) * slots)
        part = dot(value.astype(jnp.float32).astype(jnp.bfloat16), pick.astype(jnp.float32).astype(jnp.bfloat16))
        digits = part if digits is None else digits + part
    x[:, :embed] = queries[...]
    x[:, embed:] = digits.astype(jnp.bfloat16)


def prepare(queries, ids, child, cross, query, bias, scale, slots):
    embed, hidden = child.shape
    vmem = pl.BlockSpec(memory_space=pltpu.VMEM)
    place = lax.axis_index("hid").astype(jnp.int32).reshape(1)
    return pl.pallas_call(
        functools.partial(prepare_kernel, slots),
        out_shape=(
            jax.ShapeDtypeStruct((3 * embed + 16, hidden), jnp.bfloat16),
            jax.ShapeDtypeStruct((queries.shape[0], embed + DIGITS * slots), jnp.bfloat16),
        ),
        in_specs=[pl.BlockSpec(memory_space=pltpu.SMEM)] + [vmem] * 7,
        out_specs=(vmem, vmem),
        name="prepare",
    )(place, queries, ids, child, cross, query, bias.reshape(1, -1), scale.reshape(1, -1))


def shards(queries, beam_ids, child_table, w_query, w_child, w_cross, bias, w_out):
    nbeam, nhid = lax.axis_size("beam"), lax.axis_size("hid")
    qcount, width = beam_ids.shape
    embed = queries.shape[1]
    slots = width // nhid
    half = child_table.shape[0] // 2
    assert 2 * slots <= LANES and half <= 65536 and half * nbeam <= BASE**DIGITS and qcount * nbeam <= 8 * LANES

    own, x = prepare(queries, beam_ids, w_child, w_cross, w_query, bias, w_out, slots)
    weights = [own]
    for shift in range(1, nhid):
        weights.append(lax.ppermute(own, "hid", [(i, (i + shift) % nhid) for i in range(nhid)]))
    x = lax.all_gather(x, "beam", axis=0, tiled=True)

    me = lax.axis_index("beam").astype(jnp.int32).reshape(1)
    chunks, used, names, gidx, order, x = fetch(me, x, child_table.reshape(-1, 8, embed), slots, embed)
    found = score(used, names, x, gidx, order, chunks, weights, embed)[:, : 2 * slots]
    parts = lax.all_to_all(found.reshape(nbeam, qcount, 2 * slots), "beam", split_axis=0, concat_axis=0, tiled=True)
    return jnp.sum(parts, axis=0)


def solution(mesh):
    return jax.shard_map(
        shards,
        mesh=mesh,
        in_specs=(
            P("beam", None),
            P("beam", None),
            P("beam", None),
            P(None, "hid"),
            P(None, "hid"),
            P(None, "hid"),
            P("hid"),
            P("hid"),
        ),
        out_specs=P("beam", "hid"),
        check_vma=False,
    )
```

```python
import functools

import jax
import jax.numpy as jnp
from jax import lax
from jax.experimental import pallas as pl
from jax.experimental.pallas import tpu as pltpu
from jax.sharding import PartitionSpec as P

LANES = 128
TILES = 32
DIGITS = 2
BASE = 512
ROWS = 256
OUT_SLOTS = 8
IN_SLOTS = 4
GROUP = 2 * TILES
PIECE = 896


def iota(shape, dim):
    return lax.broadcasted_iota(jnp.int32, shape, dim)


def dot(a, b):
    return jnp.dot(a, b, preferred_element_type=jnp.float32)


def aligned(index, size):
    return pl.ds(pl.multiple_of(index, size), size)


def doubler():
    return (iota((2 * ROWS, ROWS), 0) >> 1 == iota((2 * ROWS, ROWS), 1)).astype(jnp.float32).astype(jnp.bfloat16)


def fetch_kernel(
    slots, embed, me_ref, x_ref, table_hbm,
    chunks_hbm, used_ref, name_hbm, gidx_hbm, order_hbm, sorted_hbm,
    name_ref, gidx, order_ref, sorted_ref, side_sem, table, table_sem, eighths, insides, most_v, most_s, most_sem, rows_v, rows_sem, names_v, name_s, name_sem,
    q2f, work, work_sem, *rows_s,
):
    queries = x_ref.shape[0]
    blocks = queries // 8
    half = table_hbm.shape[0] * 4
    table_copy = pltpu.make_async_copy(table_hbm, table, table_sem)
    table_copy.start()

    lane = iota((ROWS, LANES), 1)
    lane8 = iota((8, LANES), 1)
    pick_row, pick_lane = iota((DIGITS * slots, LANES), 0), iota((DIGITS * slots, LANES), 1)
    spread = jnp.zeros((DIGITS * slots, LANES), jnp.float32)
    for digit in range(DIGITS):
        spread = jnp.where(pick_row == (pick_lane >> 1) + digit * slots, float(BASE) ** digit, spread)
    spread = jnp.where(pick_lane < 2 * slots, spread, 0.0).astype(jnp.bfloat16)
    from_lane, to_lane = iota((LANES, LANES), 0), iota((LANES, LANES), 1)
    before = ((from_lane & 1) == 0) & ((from_lane >> 1) < (to_lane >> 1))
    before = before.astype(jnp.float32).astype(jnp.bfloat16)
    base = (me_ref[0] * half).astype(jnp.float32) - sum(BASE // 2 * BASE**digit for digit in range(DIGITS))
    twice = doubler()

    def owned_of(digits):
        local = dot(digits, spread) - base
        mine = (local >= 0.0) & (local < float(half)) & (iota(local.shape, 1) < 2 * slots)
        return local, mine

    mark = jnp.where(owned_of(x_ref[:, embed:])[1] & ((iota((queries, LANES), 1) & 1) == 0), 1.0, 0.0)
    number = jnp.sum(mark, axis=1, keepdims=True)
    across = lax.dot_general(
        jnp.ones((8, LANES), jnp.bfloat16), mark.astype(jnp.bfloat16), (((1,), (1,)), ((), ())),
        preferred_element_type=jnp.float32,
    )[0:1]
    earlier = iota((queries, queries), 1) < iota((queries, queries), 0)
    ahead = (across > number) | ((across == number) & earlier)
    order = jnp.sum(ahead.astype(jnp.float32), axis=1, keepdims=True).astype(jnp.int32)
    order_ref[...] = jnp.broadcast_to(order, (queries, LANES))
    later = iota((queries, queries), 0) < iota((queries, queries), 1)
    behind = (number > across) | ((number == across) & later)
    place = jnp.sum(behind.astype(jnp.float32), axis=0, keepdims=True).astype(jnp.int32)
    move = (iota((queries, queries), 0) == place).astype(jnp.float32).astype(jnp.bfloat16)
    sorted_ref[...] = dot(move, x_ref[...]).astype(jnp.bfloat16)
    sides = [
        pltpu.make_async_copy(value, target, side_sem.at[i])
        for i, (value, target) in enumerate(
            ((order_ref, order_hbm), (sorted_ref, sorted_hbm), (gidx, gidx_hbm), (name_ref, name_hbm))
        )
    ]
    sides[0].start()
    sides[1].start()

    def compact(step, most):
        here = aligned(step * ROWS, ROWS)
        local, owned = owned_of(sorted_ref[here, embed:])
        first = owned & ((lane & 1) == 0)
        mark = jnp.where(first, 1.0, 0.0)
        rank = dot(mark.astype(jnp.bfloat16), before).astype(jnp.int32)
        gidx[here, :] = jnp.where(owned, rank, -1)
        moved = jnp.where(first, ((lane - rank) << 16) + local.astype(jnp.int32), 0)
        for bit in range(7):
            other = pltpu.roll(moved, LANES - 2**bit, axis=1)
            flag = 65536 << bit
            moved = jnp.where((other & flag) != 0, other, jnp.where((moved & flag) != 0, 0, moved))
        total = jnp.broadcast_to(jnp.sum(mark, axis=1, keepdims=True), (ROWS, LANES)).astype(jnp.int32)
        eighth, inside = (moved & 65535) >> 2, (moved & 3) << 1
        for i in range(ROWS // 8):
            block = step * (ROWS // 8) + i
            to = aligned(block << 7, LANES)
            part = slice(i * 8, (i + 1) * 8)
            eighths[:, to] = eighth[part]
            insides[:, to] = inside[part] + (((block << 7) + lane8) << 3)
            most = jnp.where(lane8 == block, jnp.max(total[part], axis=0, keepdims=True), most)
        q2f[aligned(step * 2 * ROWS, 2 * ROWS), :] = dot(twice, sorted_ref[here, :embed])
        return most

    most_v[...] = lax.fori_loop(0, queries // ROWS, compact, jnp.zeros((8, LANES), jnp.int32))
    most_copy = pltpu.make_async_copy(most_v, most_s, most_sem)
    most_copy.start()
    sides[2].start()
    most_copy.wait()

    zero = jnp.zeros((8, LANES), jnp.int32)

    def append(block, carry):
        used, held = carry
        more = most_s[0, block]
        turn, low = used & (LANES - 1), used >> 7
        crossed = turn + more >= LANES
        kept = []
        for source, target, last in zip((eighths, insides), (rows_v, names_v), held):
            rolled = pltpu.roll(source[:, aligned(block << 7, LANES)], turn, axis=1)
            merged = jnp.where(lane8 >= turn, rolled, last)
            target[:, aligned(low << 7, LANES)] = merged
            kept.append(jnp.where(crossed, rolled, merged))
        return used + more, tuple(kept)

    used, held = lax.fori_loop(0, blocks, append, (0, (zero, zero)), unroll=16)
    for target, last in zip((rows_v, names_v), held):
        target[:, aligned((used >> 7) << 7, LANES)] = last
    chunks = (used + TILES - 1) >> (TILES.bit_length() - 1)
    used_ref[0] = chunks
    name_ref[...] = names_v[0:1, :]
    sides[3].start()

    def scalar_copies(act):
        for start in range(0, names_v.shape[1], PIECE):
            here = pl.ds(start, min(PIECE, names_v.shape[1] - start))

            @pl.when(start < chunks * TILES)
            def _():
                for s in range(8):
                    act(pltpu.make_async_copy(rows_v.at[pl.ds(s, 1), here], rows_s[s].at[:, here], rows_sem.at[s]))
                act(pltpu.make_async_copy(names_v.at[pl.ds(0, 1), here], name_s.at[:, here], name_sem))

    scalar_copies(lambda copy: copy.start())
    scalar_copies(lambda copy: copy.wait())
    table_copy.wait()

    pair = iota((8, LANES), 0) >> 1
    child = iota((8, LANES), 0) & 1

    def out_copy(number):
        slot = number & (OUT_SLOTS - 1)
        return pltpu.make_async_copy(work.at[slot], chunks_hbm.at[number], work_sem.at[slot])

    def chunk(number, carry):
        slot = number & (OUT_SLOTS - 1)

        @pl.when(number >= OUT_SLOTS)
        def _():
            out_copy(number - OUT_SLOTS).wait()

        def tile(t, carry):
            at = number * TILES + t
            block = name_s[0, at] >> 10
            names = names_v[:, aligned((at >> 7) << 7, LANES)]
            starts = jnp.take_along_axis(names, jnp.broadcast_to(at & (LANES - 1), (8, LANES)), axis=1) & 7
            halves = []
            for part in range(2):
                place = jnp.take_along_axis(starts, pair + 4 * part, axis=0) + child
                got = [None] * (embed // LANES)
                for s in range(4):
                    eight = table[rows_s[part * 4 + s][0, at]].astype(jnp.float32)
                    for j in range(embed // LANES):
                        piece = jnp.take_along_axis(eight[:, j * LANES : (j + 1) * LANES], place, axis=0)
                        got[j] = piece if s == 0 else jnp.where(pair == s, piece, got[j])
                halves.append(jnp.concatenate(got, axis=1))
            rows = jnp.concatenate(halves, axis=0)
            here = aligned(t << 4, 16)
            work[slot, here, :embed] = rows.astype(jnp.bfloat16)
            work[slot, here, embed:] = (rows * q2f[aligned(block << 4, 16), :]).astype(jnp.bfloat16)
            return carry

        lax.fori_loop(0, TILES, tile, 0, unroll=TILES)
        out_copy(number).start()
        return carry

    lax.fori_loop(0, chunks, chunk, 0)

    def drain(number, carry):
        out_copy(number).wait()
        return carry

    lax.fori_loop(jnp.maximum(chunks - OUT_SLOTS, 0), chunks, drain, 0)
    for side in sides:
        side.wait()


def fetch(me, x, table, slots, embed):
    queries = x.shape[0]
    blocks = queries // 8
    tiles = -(-(blocks * slots + 2 * LANES) // LANES) * LANES
    vmem = pl.BlockSpec(memory_space=pltpu.VMEM)
    smem = pl.BlockSpec(memory_space=pltpu.SMEM)
    anywhere = pl.BlockSpec(memory_space=pl.ANY)
    i32 = jnp.int32
    return pl.pallas_call(
        functools.partial(fetch_kernel, slots, embed),
        out_shape=(
            jax.ShapeDtypeStruct((blocks * slots // TILES, TILES * 16, 2 * embed), jnp.bfloat16),
            jax.ShapeDtypeStruct((1,), i32),
            jax.ShapeDtypeStruct((1, tiles), i32),
            jax.ShapeDtypeStruct((queries, LANES), i32),
            jax.ShapeDtypeStruct((queries, LANES), i32),
            jax.ShapeDtypeStruct(x.shape, x.dtype),
        ),
        in_specs=[smem, vmem, anywhere],
        out_specs=(anywhere, smem, anywhere, anywhere, anywhere, anywhere),
        scratch_shapes=[
            pltpu.VMEM((1, tiles), i32),
            pltpu.VMEM((queries, LANES), i32),
            pltpu.VMEM((queries, LANES), i32),
            pltpu.VMEM(x.shape, x.dtype),
            pltpu.SemaphoreType.DMA((4,)),
            pltpu.VMEM(table.shape, table.dtype),
            pltpu.SemaphoreType.DMA(()),
            pltpu.VMEM((8, blocks * LANES), i32),
            pltpu.VMEM((8, blocks * LANES), i32),
            pltpu.VMEM((8, LANES), i32),
            pltpu.SMEM((8, LANES), i32),
            pltpu.SemaphoreType.DMA(()),
            pltpu.VMEM((8, tiles), i32),
            pltpu.SemaphoreType.DMA((8,)),
            pltpu.VMEM((8, tiles), i32),
            pltpu.SMEM((1, tiles), i32),
            pltpu.SemaphoreType.DMA(()),
            pltpu.VMEM((2 * queries, embed), jnp.float32),
            pltpu.VMEM((OUT_SLOTS, TILES * 16, 2 * embed), jnp.bfloat16),
            pltpu.SemaphoreType.DMA((OUT_SLOTS,)),
        ]
        + [pltpu.SMEM((1, tiles), i32)] * 8,
        cost_estimate=pl.CostEstimate(flops=2 * 10**10, bytes_accessed=4 * 10**7, transcendentals=0),
        name="fetch",
    )(me, x, table)


def score_kernel(embed, used_ref, name_s, x_hbm, gidx_hbm, order_hbm, chunks_hbm, *rest):
    count = len(rest) - 14
    weights = rest[:count]
    out_ref, x_ref, gidx, order_ref, side_sem, held, held_sem, qp2, work, work_sem, scores, pending, sums, placed = rest[count:]
    queries = x_hbm.shape[0]
    hidden = weights[0].shape[1]
    sides = [
        pltpu.make_async_copy(source, value, side_sem.at[i])
        for i, (source, value) in enumerate(((x_hbm, x_ref), (gidx_hbm, gidx), (order_hbm, order_ref)))
    ]
    sides[0].start()
    copies = [pltpu.make_async_copy(weights[k], held.at[k], held_sem.at[k]) for k in range(count)]
    for copy in copies:
        copy.start()
    chunks = (used_ref[0] * TILES + GROUP - 1) // GROUP

    def in_copy(number):
        slot = number & (IN_SLOTS - 1)
        return pltpu.make_async_copy(chunks_hbm.at[number], work.at[slot], work_sem.at[slot])

    for number in range(IN_SLOTS - 1):

        @pl.when(number < chunks)
        def _():
            in_copy(number).start()

    for copy in copies:
        copy.wait()

    for side in sides[1:]:
        side.start()
    sides[0].wait()

    twice = doubler()

    def project(step, carry):
        here = aligned(step * 2 * ROWS, 2 * ROWS)
        doubled = dot(twice, x_ref[aligned(step * ROWS, ROWS), :embed]).astype(jnp.bfloat16)
        for k in range(count):
            last = held[k, 3 * embed :, :].astype(jnp.float32)
            bias = last[0:1] + last[1:2] + last[2:3]
            qp2[here, k * hidden : (k + 1) * hidden] = dot(doubled, held[k, 2 * embed : 3 * embed, :]) + bias
        return carry

    lax.fori_loop(0, queries // ROWS, project, 0, unroll=2)

    lane16 = iota((16, LANES), 1)

    def scale_of(k):
        last = held[k, 3 * embed :, :].astype(jnp.float32)
        return last[3:4] + last[4:5] + last[5:6]

    def activate(pre, name, k):
        own = qp2[aligned((name >> 10) << 4, 16), k * hidden : (k + 1) * hidden]
        act = jnp.maximum(pre + own, 0.0) * scales[k]
        total = act[:, :LANES]
        for j in range(LANES, hidden, LANES):
            total = total + act[:, j : j + LANES]
        return total

    def finish(number):
        for t in range(GROUP):
            name = name_s[0, number * GROUP + t]
            part = slice(t * 16, (t + 1) * 16)
            total = activate(pending[part, :], name, count - 1)
            if count > 1:
                total = total + sums[part, :]
            here = aligned((name >> 10) << 4, 16)
            rank = (name >> 3) & (LANES - 1)
            scores[here, :] = jnp.where(lane16 == rank, jnp.sum(total, axis=1, keepdims=True), scores[here, :])

    scales = [scale_of(k) for k in range(count)]

    def score_chunk(number, carry):
        ahead = number + IN_SLOTS - 1

        @pl.when(ahead < chunks)
        def _():
            in_copy(ahead).start()

        in_copy(number).wait()
        rows = work.at[number & (IN_SLOTS - 1)]
        totals = [None] * GROUP
        for k in range(count - 1):
            pre = dot(rows[...], held[k, : 2 * embed, :])
            if k == 0:
                finish(jnp.maximum(number - 1, 0))
            for t in range(GROUP):
                own = activate(pre[t * 16 : (t + 1) * 16], name_s[0, number * GROUP + t], k)
                totals[t] = own if k == 0 else totals[t] + own
        if count > 1:
            for t in range(GROUP):
                sums[t * 16 : (t + 1) * 16, :] = totals[t]
        pending[...] = dot(rows[...], held[count - 1, : 2 * embed, :])
        return carry

    lax.fori_loop(0, chunks, score_chunk, 0)
    finish(jnp.maximum(chunks - 1, 0))

    for side in sides[1:]:
        side.wait()
    lane8 = iota((8, LANES), 1)

    def place(block):
        index = gidx[aligned(block << 3, 8), :]
        safe = jnp.maximum(index, 0)
        left = jnp.take_along_axis(scores[pl.ds(block * 16, 8, stride=2), :], safe, axis=1)
        right = jnp.take_along_axis(scores[pl.ds(block * 16 + 1, 8, stride=2), :], safe, axis=1)
        return jnp.where(index < 0, 0.0, jnp.where((lane8 & 1) == 0, left, right))

    def place_block(block, carry):
        placed[aligned(block << 3, 8), :] = place(block)
        return carry

    lax.fori_loop(0, queries // 8, place_block, 0, unroll=16)

    move = (order_ref[:, 0:1] == iota((queries, queries), 1)).astype(jnp.float32).astype(jnp.bfloat16)
    left = placed[...]
    moved = None
    for _ in range(3):
        taken = left.astype(jnp.bfloat16)
        left = left - taken.astype(jnp.float32)
        part = dot(move, taken)
        moved = part if moved is None else moved + part
    out_ref[...] = moved


def score(used, names, x, gidx, order, chunks, weights, embed):
    queries = x.shape[0]
    depth, hidden = weights[0].shape
    vmem = pl.BlockSpec(memory_space=pltpu.VMEM)
    smem = pl.BlockSpec(memory_space=pltpu.SMEM)
    anywhere = pl.BlockSpec(memory_space=pl.ANY)
    return pl.pallas_call(
        functools.partial(score_kernel, embed),
        out_shape=jax.ShapeDtypeStruct((queries, LANES), jnp.float32),
        in_specs=[smem, smem, anywhere, anywhere, anywhere, anywhere] + [anywhere] * len(weights),
        out_specs=vmem,
        scratch_shapes=[
            pltpu.VMEM(x.shape, x.dtype),
            pltpu.VMEM((queries, LANES), jnp.int32),
            pltpu.VMEM((queries, LANES), jnp.int32),
            pltpu.SemaphoreType.DMA((3,)),
            pltpu.VMEM((len(weights), depth, hidden), jnp.bfloat16),
            pltpu.SemaphoreType.DMA((len(weights),)),
            pltpu.VMEM((2 * queries, len(weights) * hidden), jnp.float32),
            pltpu.VMEM((IN_SLOTS, GROUP * 16, 2 * embed), jnp.bfloat16),
            pltpu.SemaphoreType.DMA((IN_SLOTS,)),
            pltpu.VMEM((2 * queries, LANES), jnp.float32),
            pltpu.VMEM((GROUP * 16, hidden), jnp.float32),
            pltpu.VMEM((GROUP * 16, LANES), jnp.float32),
            pltpu.VMEM((queries, LANES), jnp.float32),
        ],
        name="score",
    )(used, names, x, gidx, order, chunks.reshape(-1, GROUP * 16, 2 * embed), *weights)


def prepare_kernel(slots, place_ref, queries, ids, child, cross, query, bias, scale, own, x):
    embed = queries.shape[1]
    for k, w in enumerate((child, cross, query)):
        own[k * embed : (k + 1) * embed, :] = w[...]
    row = iota((16, own.shape[1]), 0)
    tail = jnp.zeros((16, own.shape[1]), jnp.float32)
    for k, value in enumerate((bias, scale)):
        left = value[...]
        for part in range(3):
            taken = left.astype(jnp.bfloat16).astype(jnp.float32)
            tail = jnp.where(row == 3 * k + part, taken, tail)
            left = left - taken
    own[3 * embed :, :] = tail.astype(jnp.bfloat16)
    shape = (ids.shape[1], DIGITS * slots)
    digits = None
    for digit in range(DIGITS):
        value = ((ids[...] >> (digit * (BASE.bit_length() - 1))) & (BASE - 1)) - BASE // 2
        pick = iota(shape, 0) - place_ref[0] * slots == iota(shape, 1) - digit * slots
        pick = pick & (iota(shape, 1) >= digit * slots) & (iota(shape, 1) < (digit + 1) * slots)
        part = dot(value.astype(jnp.float32).astype(jnp.bfloat16), pick.astype(jnp.float32).astype(jnp.bfloat16))
        digits = part if digits is None else digits + part
    x[:, :embed] = queries[...]
    x[:, embed:] = digits.astype(jnp.bfloat16)


def prepare(queries, ids, child, cross, query, bias, scale, slots):
    embed, hidden = child.shape
    vmem = pl.BlockSpec(memory_space=pltpu.VMEM)
    place = lax.axis_index("hid").astype(jnp.int32).reshape(1)
    return pl.pallas_call(
        functools.partial(prepare_kernel, slots),
        out_shape=(
            jax.ShapeDtypeStruct((3 * embed + 16, hidden), jnp.bfloat16),
            jax.ShapeDtypeStruct((queries.shape[0], embed + DIGITS * slots), jnp.bfloat16),
        ),
        in_specs=[pl.BlockSpec(memory_space=pltpu.SMEM)] + [vmem] * 7,
        out_specs=(vmem, vmem),
        name="prepare",
    )(place, queries, ids, child, cross, query, bias.reshape(1, -1), scale.reshape(1, -1))


def shards(queries, beam_ids, child_table, w_query, w_child, w_cross, bias, w_out):
    nbeam, nhid = lax.axis_size("beam"), lax.axis_size("hid")
    qcount, width = beam_ids.shape
    embed = queries.shape[1]
    slots = width // nhid
    half = child_table.shape[0] // 2
    assert 2 * slots <= LANES and half <= 65536 and half * nbeam <= BASE**DIGITS and qcount * nbeam <= 8 * LANES

    own, x = prepare(queries, beam_ids, w_child, w_cross, w_query, bias, w_out, slots)
    weights = [own]
    for shift in range(1, nhid):
        weights.append(lax.ppermute(own, "hid", [(i, (i + shift) % nhid) for i in range(nhid)]))
    x = lax.all_gather(x, "beam", axis=0, tiled=True)

    me = lax.axis_index("beam").astype(jnp.int32).reshape(1)
    chunks, used, names, gidx, order, x = fetch(me, x, child_table.reshape(-1, 8, embed), slots, embed)
    found = score(used, names, x, gidx, order, chunks, weights, embed)[:, : 2 * slots]
    parts = lax.all_to_all(found.reshape(nbeam, qcount, 2 * slots), "beam", split_axis=0, concat_axis=0, tiled=True)
    return jnp.sum(parts, axis=0)


def solution(mesh):
    return jax.shard_map(
        shards,
        mesh=mesh,
        in_specs=(
            P("beam", None),
            P("beam", None),
            P("beam", None),
            P(None, "hid"),
            P(None, "hid"),
            P(None, "hid"),
            P("hid"),
            P("hid"),
        ),
        out_specs=P("beam", "hid"),
        check_vma=False,
    )
```
